128 devices in a mesh: px: 8 (over y_lo, x), py: 16 (over z, y_hi, core).
Axes of the slice: x: 4, y: 4 (y_hi: 2, y_lo: 2; y = y_hi * 2 + y_lo), z: 4, core: 2. Of those that a mesh axis runs over, the one named last changes fastest.
Arguments:
- photons: float32 [4096, 128], P(('px', 'py')), may hold values from 50 to 1000
- halo_cells: int32 [4096, 128], P(('px', 'py')), may hold values from 0 to 442367
- halo_counts: int32 [4096], P(('px', 'py')), may hold values from 1 to 128
- owners: int32 [4096, 1], P(('px', 'py')), may hold values from 0 to 15; in each aligned block of 32 rows (0 to 31, 32 to 63, ...) at most 4 rows name the same one
- density: float32 [384, 384, 384], P('px', 'py'), may hold values from 0.02 to 50
Outputs:
- fraction: float32 [384, 384, 384], P('px', 'py')
The draws below stay inside these ranges and needn't reach their ends.
Inputs may be any that keep to these rules, and one draw needn't show every extreme that they name: The halos of a block all lie in pencil owners[b] of the block's own slab. Among the 32 blocks of one device no owner appears more than 4 times, a bound that some block reaches. Slots at or past halo_counts[b] are not live and carry arbitrary values. `halo_cells`: A cell index within the owner pencil is (x * 24 + y) * 384 + z with x, y, z local to that pencil.
All inputs are finite; a program needn't handle non-finite values.
Results may differ from the reference program's by a relative error of at most 0.0003.
Values sent between devices are 32-bit elements; how exact they have to be, the bound alone decides.
No kernel may reach another device: no remote copies, remote signals or barrier semaphores. Data moves between devices by JAX's collectives and lax.ppermute only.
A program may use at most 128 MiB of HBM per device.

```python
import math
import jax
import jax.numpy as jnp
import numpy as np
from jax import lax

NG = 384
SLOTS = 128
CAP = 4
RADIUS = 20
BLK_DEV = 32
CX = 48
CY = 24
HROWS = 4096
N_PY = 16


def draw_density(key, part):
    subkeys = jax.random.split(jax.random.fold_in(key, 7), 4)
    wave_numbers = jax.random.randint(subkeys[0], (4, 3), 1, 4)
    flip_signs = jax.random.randint(subkeys[1], (4, 3), 0, 2) * 2 - 1
    wave_numbers = wave_numbers * flip_signs
    phases = jax.random.uniform(subkeys[2], (4,), jnp.float32, -jnp.pi, jnp.pi)
    coords = jnp.arange(NG, dtype=jnp.int32)
    smooth = jnp.zeros((NG, NG, NG), jnp.float32)
    for number in range(4):
        along_x = wave_numbers[number, 0] * coords % NG
        along_y = wave_numbers[number, 1] * coords % NG
        along_z = wave_numbers[number, 2] * coords % NG
        total = (along_x[:, None, None] + along_y[None, :, None] + along_z[None, None, :]) % NG
        smooth = smooth + jnp.cos(total.astype(jnp.float32) * (2.0 * jnp.pi / NG) + phases[number])
    smooth = smooth / jnp.sqrt(2.0)
    rough_part = jnp.clip(1.8 * jax.random.normal(subkeys[3], (NG, NG, NG), jnp.float32), -4.0, 4.0) - 1.4
    amplitude = 0.8
    return jnp.clip(jnp.exp(amplitude * smooth + rough_part), 0.02, 50.0).astype(jnp.float32)


def place_ends(result, own_key, smallest, top_value):
    spot = [jax.random.randint(jax.random.fold_in(own_key, axis), (), 0, length) for axis, length in enumerate(result.shape)]
    main_axis = result.shape.index(max(result.shape))
    neighbour = spot[:main_axis] + [(spot[main_axis] + 1) % result.shape[main_axis]] + spot[main_axis + 1:]
    return result.at[tuple(spot)].set(smallest).at[tuple(neighbour)].set(top_value)


def level_of(key, extent, pieces, low, largest):
    factor_of = 1.0
    for axis_at, shards_of in pieces:
        heights = jax.random.uniform(jax.random.fold_in(jax.random.fold_in(key, 6), axis_at), (shards_of,), jnp.float32, low / len(pieces), largest / len(pieces))
        factor_of = factor_of * jnp.repeat(jnp.exp(heights), extent[axis_at] // shards_of).reshape((-1,) + (1,) * (len(extent) - 1 - axis_at))
    return factor_of


def deal_out(stream_key, own, number, rows, amount, top, most, skew):
    sequence = jax.random.permutation(stream_key, amount)
    crowded, usual = shares(amount, rows * top, most, skew, True), shares(amount, rows * top, most, skew, False)
    places = jnp.arange(amount)

    def named(sizes, rotation):
        used = int((sizes > 0).sum())
        fixed = max(1, used // 4)
        passed = fixed + (places - fixed + rotation * (used - fixed)) % max(1, amount - fixed)
        return jnp.zeros((amount,), jnp.int32).at[sequence[jnp.where(places < fixed, places, passed)]].set(jnp.asarray(sizes, jnp.int32))

    sizes = jnp.where(number % 4 == 0, named(crowded, number // 4), named(usual, number - number // 4 - 1))
    mixed = jax.random.permutation(jax.random.fold_in(own, 3), amount)
    giver, receiver = mixed[0:amount // 2 * 2:2], mixed[1:amount // 2 * 2:2]
    margin = jnp.minimum(sizes[giver] - 1, most - sizes[receiver]) // 2
    margin = jnp.where((giver == sequence[0]) | (receiver == sequence[0]) | (sizes[receiver] == 0), 0, jnp.maximum(margin, 0))
    passed = jax.random.randint(jax.random.fold_in(own, 4), (amount // 2,), 0, 1 << 20) % (margin + 1)
    sizes = sizes.at[giver].add(-passed).at[receiver].add(passed)
    items = jnp.searchsorted(jnp.cumsum(sizes), jnp.arange(rows * top), side="right").astype(jnp.int32)
    table = items.reshape(top, rows).T
    table = table[jax.random.permutation(jax.random.fold_in(own, 1), rows)]
    rotation = jax.random.randint(jax.random.fold_in(own, 2), (rows, 1), 0, top)
    return jnp.take_along_axis(table, (jnp.arange(top)[None, :] + rotation) % top, axis=1)


def shares(count, total, reach, slope, full):
    weights = [(1 << 20) // math.isqrt(rank ** slope) + 1 for rank in range(1, count + 1)]
    largest = reach if full else min(reach, max(-(-total // count), total * weights[0] // sum(weights)))
    least = 1 if total - largest >= count - 1 else 0
    counts, spare = [largest] + [least] * (count - 1), total - largest - least * (count - 1)
    while spare > 0:
        free = [i for i in range(1, count) if counts[i] < largest] or [i for i in range(1, count) if counts[i] < reach]
        whole, budget = sum([weights[i] for i in free]), spare
        for i in free:
            extra = min(reach - counts[i], max(1, budget * weights[i] // whole), spare)
            counts[i] = counts[i] + extra
            spare = spare - extra
    return np.array(counts)


def setup_inputs(seed: int = 0) -> dict:
    seeds = jax.random.split(jax.random.key(seed), 6)
    photons = jnp.clip(jnp.exp(math.log(1000.0) - 2.9957323 * jax.random.uniform(seeds[0], (HROWS, SLOTS), jnp.float32) ** level_of(seeds[0], (HROWS, SLOTS), ((0, 128),), -0.2, 0.2)), 50.0, 1000.0)
    halo_cells = place_ends(jax.random.randint(seeds[1], (HROWS, SLOTS), 0, CX * CY * NG), jax.random.fold_in(seeds[1], 1), 0, (CX * CY * NG) - 1).astype(jnp.int32)
    halo_counts = place_ends(jax.random.randint(seeds[2], (HROWS,), 1, SLOTS + 1), jax.random.fold_in(seeds[2], 1), 1, SLOTS).astype(jnp.int32)
    owners_keys = jax.random.split(jax.random.fold_in(seeds[3], 1), HROWS // BLK_DEV)
    owners_turns = jax.random.permutation(jax.random.fold_in(seeds[3], 3), HROWS // BLK_DEV)
    owners = jax.vmap(lambda own, number: deal_out(jax.random.fold_in(seeds[3], 2), own, number, BLK_DEV, N_PY, 1, CAP, 2))(owners_keys, owners_turns).reshape((HROWS, 1))
    density = draw_density(jax.random.fold_in(seeds[5], 71), 0)
    return dict(photons=photons, halo_cells=halo_cells, halo_counts=halo_counts, owners=owners, density=density)


def top_hat(freq_x, freq_y, freq_z):
    radial = jnp.sqrt(freq_x * freq_x + freq_y * freq_y + freq_z * freq_z) * (2.0 * jnp.pi * RADIUS / NG)
    safe = jnp.where(radial > 0, radial, 1.0)
    value = 3.0 * (jnp.sin(safe) - safe * jnp.cos(safe)) / (safe * safe * safe)
    return jnp.where(radial > 0, value, 1.0)

def reference(photons, halo_cells, halo_counts, owners, density):
    row_count = photons.shape[0]
    row_index = jnp.arange(row_count, dtype=jnp.int32)
    slab_index = row_index // (N_PY * BLK_DEV)
    local_x = halo_cells // (CY * NG)
    local_y = halo_cells // NG % CY
    local_z = halo_cells % NG
    global_x = slab_index[:, None] * CX + local_x
    global_y = owners[:, 0:1] * CY + local_y
    flat_index = ((global_x * NG + global_y) * NG + local_z).astype(jnp.int32)
    live_slots = jnp.arange(photons.shape[1], dtype=jnp.int32)[None, :] < halo_counts[:, None]
    weights = jnp.where(live_slots, photons, jnp.zeros_like(photons))
    field = jnp.zeros((NG * NG * NG,), photons.dtype).at[flat_index.reshape(-1)].add(weights.reshape(-1))
    field = field.reshape(NG, NG, NG)
    packed = lax.complex(field, density)
    spectrum = jnp.fft.fftn(packed)
    index_values = jnp.arange(NG, dtype=jnp.int32)
    signed_frequency = jnp.where(index_values < NG // 2, index_values, index_values - NG).astype(density.dtype)
    window = top_hat(signed_frequency[:, None, None], signed_frequency[None, :, None], signed_frequency[None, None, :])
    smoothed = jnp.fft.ifftn(spectrum * window)
    photon_smooth = jnp.real(smoothed)
    density_smooth = jnp.imag(smoothed)
    fraction = jnp.clip(photon_smooth / jnp.maximum(density_smooth, 0.5), 0.0, 1.0)
    return fraction.astype(jnp.float32)
```

```python
import math

import jax
import jax.numpy as jnp
import ml_dtypes
import numpy as np
from jax import lax
from jax.experimental import pallas as pl
from jax.experimental.pallas import tpu as pltpu
from jax.sharding import PartitionSpec as P

NG = 384
SLOTS = 128
CAP = 4
RADIUS = 20
N_PX = 8
N_PY = 16
N_DEV = 128
CX = 48
CY = 24
ROWS = CX * CY
LB = ROWS // 128
AXES = ("px", "py")
BF = jnp.bfloat16
F32 = jnp.float32


def split_np(table):
    high = table.astype(ml_dtypes.bfloat16)
    low = (table - high.astype(np.float64)).astype(ml_dtypes.bfloat16)
    return high, low


def plane_tables():
    z = np.arange(NG)

    def rows(kz):
        angle = 2.0 * np.pi * ((kz * z) % NG) / NG
        return np.cos(angle), np.sin(angle)

    t_a = np.zeros((2, N_DEV, NG))
    t_bd = np.zeros((2, N_DEV, NG))
    t_bs = np.zeros((2, N_DEV, NG))
    t_c = np.zeros((2, N_DEV, NG))
    for d in range(N_DEV):
        t_a[0, d], t_a[1, d] = rows(d + 1)
        t_c[0, d], t_c[1, d] = rows(64 + d)
        if d < 63:
            t_bd[0, d], t_bd[1, d] = rows(129 + d)
        elif d < 126:
            t_bs[0, d], t_bs[1, d] = rows(d - 62)
        else:
            even = rows(0 if d == 126 else NG // 2)[0]
            t_bs[0, d] = even
            t_bd[1, d] = even
    return tuple(split_np(t.reshape(2 * N_DEV, NG)) for t in (t_a, t_bd, t_bs, t_c))


def real_form(cos_part, sin_part):
    return np.block([[cos_part, sin_part], [-sin_part, cos_part]])


def device_table():
    s = np.arange(N_DEV)
    i, q = s // N_PY, s % N_PY
    frac = np.outer(i, i) / N_PX + np.outer(q, q) / N_PY
    angle = 2.0 * np.pi * (frac % 1.0)
    return split_np(real_form(np.cos(angle), np.sin(angle)))


def lane_table():
    m = np.arange(NG)
    b, y = m // CY, m % CY
    frac = np.outer(b, b) / 16.0 + np.outer(y, y) / CY
    angle = 2.0 * np.pi * (frac % 1.0)
    return split_np(real_form(np.cos(angle), np.sin(angle)).T)


def twiddles():
    k = np.arange(N_DEV)
    kx, ky = k // N_PY, k % N_PY
    r = np.arange(ROWS)
    x, y = r // CY, r % CY
    angle = 2.0 * np.pi * ((np.outer(kx, x) + np.outer(ky, y)) % NG) / NG
    u = np.arange(3)
    b = np.arange(NG) // CY
    angle2 = 2.0 * np.pi * ((np.outer(u, b)) % 48) / 48.0
    tw1 = np.stack([np.cos(angle), np.sin(angle)]).astype(np.float32)
    tw2 = np.concatenate([np.cos(angle2), np.sin(angle2), np.zeros((2, NG))]).astype(np.float32)
    return tw1, tw2


def window(kz):
    row = lax.broadcasted_iota(jnp.int32, (NG, NG), 0)
    lane = lax.broadcasted_iota(jnp.int32, (NG, NG), 1)
    u, k1 = row // N_DEV, row % N_DEV
    kx = k1 // N_PY + N_PX * (u + 3 * (lane // CY))
    ky = k1 % N_PY + N_PY * (lane % CY)
    fx = jnp.where(kx < NG // 2, kx, kx - NG)
    fy = jnp.where(ky < NG // 2, ky, ky - NG)
    square = (fx * fx + fy * fy + kz * kz).astype(F32)
    radial = jnp.sqrt(square) * (2.0 * jnp.pi * RADIUS / NG)
    safe = jnp.where(radial > 0, radial, 1.0)
    value = 3.0 * (jnp.sin(safe) - safe * jnp.cos(safe)) / (safe * safe * safe)
    value = jnp.where(radial > 0, value, 1.0)
    both = (kz > 0) & (kz < NG // 2)
    return value * (jnp.where(both, 2.0, 1.0) / float(NG) ** 3)


def split(value):
    high = value.astype(BF)
    return high, (value - high.astype(F32)).astype(BF)


def dot(left, right, dims=((1,), (0,))):
    return lax.dot_general(left, right, (dims, ((), ())), preferred_element_type=F32)


def dot3(left, right, dims=((1,), (0,))):
    return (
        dot(left[0], right[0], dims) + dot(left[1], right[0], dims) + dot(left[0], right[1], dims)
    )


def sort_kernel(photons, cells, counts, owners, out):
    blocks = photons.shape[0]
    lane = lax.broadcasted_iota(jnp.int32, (blocks, SLOTS), 1)
    live = lane < counts[...]
    weight = jnp.where(live, photons[...], 0.0)
    where = jnp.where(live, cells[...], 0).astype(F32)
    hot = jnp.where(lane == owners[...], 1.0, 0.0)
    tri = jnp.where(
        lax.broadcasted_iota(jnp.int32, (blocks, blocks), 0)
        >= lax.broadcasted_iota(jnp.int32, (blocks, blocks), 1),
        1.0,
        0.0,
    )
    rank = jnp.sum(dot(tri.astype(BF), hot.astype(BF)) * hot, axis=1, keepdims=True) - 1.0
    place = owners[...] * CAP + rank.astype(jnp.int32)
    place_hot = jnp.where(lane == place, 1.0, 0.0).astype(BF)
    slots = N_PY * CAP
    for half, value in enumerate((weight, where)):
        first, rest = value.astype(BF), value
        total = None
        for _ in range(3):
            first = rest.astype(BF)
            rest = rest - first.astype(F32)
            part = dot(place_hot, first, ((0,), (0,)))
            total = part if total is None else total + part
        out[pl.ds(half, slots, stride=2), :] = total[:slots]


def z_first_kernel(density, t_high, t_low, out):
    high, low = split(density[...])
    planes = dot3((t_high[...], t_low[...]), (high, low), ((1,), (1,)))
    store_rows(out, planes, 0, 2 * LB)


def store_rows(out, planes, base, pitch):
    for c in range(2):
        for j in range(LB):
            out[pl.ds(base + c * LB + j, N_DEV, stride=pitch), :] = planes[
                c * N_DEV : (c + 1) * N_DEV, j * 128 : (j + 1) * 128
            ]


def paint_kernel(weights, cells, counts, density, *rest):
    tables, (out, field, high, low) = rest[:6], rest[6:]
    (bd_high, bd_low, bs_high, bs_low, c_high, c_low) = tables
    step = 8
    field[...] = jnp.zeros(field.shape, F32)
    lane = lax.broadcasted_iota(jnp.int32, (1, 128), 1)

    def block(index, carry):
        def some(part, inner):
            for k in range(step):
                cell = cells[index, part * step + k]
                value = weights[index, part * step + k]
                row = lax.shift_right_logical(cell, 7)
                here = lane == (cell & 127)
                field[pl.ds(row, 1), :] += jnp.where(here, value, 0.0)
            return inner

        return lax.fori_loop(0, (counts[index] + step - 1) // step, some, carry)

    lax.fori_loop(0, counts.shape[0], block, 0)
    for k in range(3):
        part_high, part_low = split(field[pl.ds(k, ROWS, stride=3), :])
        high[:, k * 128 : (k + 1) * 128] = part_high
        low[:, k * 128 : (k + 1) * 128] = part_low
    source = (high[...], low[...])
    nt = ((1,), (1,))
    planes = dot3((bs_high[...], bs_low[...]), source, nt)
    planes = planes + dot3((bd_high[...], bd_low[...]), split(density[...]), nt)
    store_rows(out, planes, 0, 4 * LB)
    store_rows(out, dot3((c_high[...], c_low[...]), source, nt), 2 * LB, 4 * LB)


HALF_ROOT3 = math.sqrt(3.0) / 2.0


def middle_kernel(planes, got, dev_high, dev_low, lane_high, lane_low, tw1, tw2, win, out,
                  work, r_high, r_low, l_high, l_low):
    pitch = planes * 2 * LB
    nt = ((1,), (1,))
    for p in range(planes):
        for c in range(2):
            for j in range(LB):
                high, low = split(got[pl.ds((p * 2 + c) * LB + j, N_DEV, stride=pitch), :])
                r_high[c * N_DEV : (c + 1) * N_DEV, j * 128 : (j + 1) * 128] = high
                r_low[c * N_DEV : (c + 1) * N_DEV, j * 128 : (j + 1) * 128] = low
        dev = (dev_high[...], dev_low[...])
        for a in range(3):
            at = slice(a * NG, (a + 1) * NG)
            work[:, at] = dot3(dev, (r_high[:, at], r_low[:, at]))

        def forward(block, carry):
            rows = pl.ds(pl.multiple_of(block * 16, 16), 16)
            rows_im = pl.ds(pl.multiple_of(block * 16 + N_DEV, 16), 16)
            re, im = [], []
            for a in range(3):
                at = slice(a * NG, (a + 1) * NG)
                cos, sin = tw1[0, rows, at], tw1[1, rows, at]
                x, y = work[rows, at], work[rows_im, at]
                re.append(x * cos + y * sin)
                im.append(y * cos - x * sin)
            t_re, t_im = re[1] + re[2], im[1] + im[2]
            d_re, d_im = (re[1] - re[2]) * HALF_ROOT3, (im[1] - im[2]) * HALF_ROOT3
            m_re, m_im = re[0] - 0.5 * t_re, im[0] - 0.5 * t_im
            y_re = (re[0] + t_re, m_re + d_im, m_re - d_im)
            y_im = (im[0] + t_im, m_im - d_re, m_im + d_re)
            for u in range(3):
                cos, sin = tw2[u : u + 1, :], tw2[3 + u : 4 + u, :]
                value_re = y_re[u] * cos + y_im[u] * sin
                value_im = y_im[u] * cos - y_re[u] * sin
                to = pl.ds(pl.multiple_of(block * 16 + u * N_DEV, 16), 16)
                l_high[to, :NG], l_low[to, :NG] = split(value_re)
                l_high[to, NG:], l_low[to, NG:] = split(value_im)
            return carry

        lax.fori_loop(0, N_DEV // 16, forward, 0)
        mat = (lane_high[...], lane_low[...])
        for u in range(3):
            at = slice(u * N_DEV, (u + 1) * N_DEV)
            value = dot3((l_high[at, :], l_low[at, :]), mat)
            w = win[p, at, :]
            l_high[at, :NG], l_low[at, :NG] = split(value[:, :NG] * w)
            l_high[at, NG:], l_low[at, NG:] = split(value[:, NG:] * w)
            value = dot3((l_high[at, :], l_low[at, :]), mat, nt)
            work[0:N_DEV, u * NG : (u + 1) * NG] = value[:, :NG]
            work[N_DEV:, u * NG : (u + 1) * NG] = value[:, NG:]

        def backward(block, carry):
            rows = pl.ds(pl.multiple_of(block * 16, 16), 16)
            rows_im = pl.ds(pl.multiple_of(block * 16 + N_DEV, 16), 16)
            re, im = [], []
            for u in range(3):
                at = slice(u * NG, (u + 1) * NG)
                cos, sin = tw2[u : u + 1, :], tw2[3 + u : 4 + u, :]
                x, y = work[rows, at], work[rows_im, at]
                re.append(x * cos - y * sin)
                im.append(y * cos + x * sin)
            t_re, t_im = re[1] + re[2], im[1] + im[2]
            d_re, d_im = (re[1] - re[2]) * HALF_ROOT3, (im[1] - im[2]) * HALF_ROOT3
            m_re, m_im = re[0] - 0.5 * t_re, im[0] - 0.5 * t_im
            y_re = (re[0] + t_re, m_re - d_im, m_re + d_im)
            y_im = (im[0] + t_im, m_im + d_re, m_im - d_re)
            for a in range(3):
                at = slice(a * NG, (a + 1) * NG)
                cos, sin = tw1[0, rows, at], tw1[1, rows, at]
                r_high[rows, at], r_low[rows, at] = split(y_re[a] * cos - y_im[a] * sin)
                r_high[rows_im, at], r_low[rows_im, at] = split(y_im[a] * cos + y_re[a] * sin)
            return carry

        lax.fori_loop(0, N_DEV // 16, backward, 0)
        tn = ((0,), (0,))
        for a in range(3):
            at = slice(a * NG, (a + 1) * NG)
            value = dot3(dev, (r_high[:, at], r_low[:, at]), tn)
            for c in range(2):
                for j in range(3):
                    out[pl.ds((p * 2 + c) * LB + a * 3 + j, N_DEV, stride=pitch), :] = value[
                        c * N_DEV : (c + 1) * N_DEV, j * 128 : (j + 1) * 128
                    ]


def load_rows(got, base, pitch):
    parts = [
        jnp.concatenate(
            [got[pl.ds(base + c * LB + j, N_DEV, stride=pitch), :] for j in range(LB)], axis=1
        )
        for c in range(2)
    ]
    return split(jnp.concatenate(parts, axis=0))


def z_last_kernel(got_a, got_bc, *rest):
    tables, out = rest[:8], rest[8]
    (a_high, a_low, bd_high, bd_low, bs_high, bs_low, c_high, c_low) = tables
    tn = ((0,), (0,))
    part_a = load_rows(got_a, 0, 2 * LB)
    part_b = load_rows(got_bc, 0, 4 * LB)
    part_c = load_rows(got_bc, 2 * LB, 4 * LB)
    for k in range(LB):
        at = slice(k * 128, (k + 1) * 128)

        def pick(part):
            return part[0][:, at], part[1][:, at]

        dens = dot3(pick(part_a), (a_high[...], a_low[...]), tn)
        dens = dens + dot3(pick(part_b), (bd_high[...], bd_low[...]), tn)
        phot = dot3(pick(part_b), (bs_high[...], bs_low[...]), tn)
        phot = phot + dot3(pick(part_c), (c_high[...], c_low[...]), tn)
        out[at, :] = jnp.clip(phot / jnp.maximum(dens, 0.5), 0.0, 1.0)


def shape(*dims, dtype=F32):
    return jax.ShapeDtypeStruct(dims, dtype)


def exchange(rows, planes):
    width = planes * 2 * ROWS
    send = rows.reshape(N_DEV, 1, width)
    return lax.all_to_all(send, AXES, 0, 0, tiled=True).reshape(N_DEV * width // 128, 128)


def middle(got, planes, dev, lanes, tw, win):
    import functools

    return pl.pallas_call(
        functools.partial(middle_kernel, planes),
        out_shape=shape(N_DEV * planes * 2 * LB, 128),
        scratch_shapes=[
            pltpu.VMEM((2 * N_DEV, ROWS), F32),
            pltpu.VMEM((2 * N_DEV, ROWS), BF),
            pltpu.VMEM((2 * N_DEV, ROWS), BF),
            pltpu.VMEM((NG, 2 * NG), BF),
            pltpu.VMEM((NG, 2 * NG), BF),
        ],
        name=f"middle{planes}",
    )(got, *dev, *lanes, *tw, win)


def on_device(photons, halo_cells, halo_counts, owners, density):
    rows_density = density.reshape(ROWS, NG)
    t_a, t_bd, t_bs, t_c = plane_tables()
    dev, lanes, tw = device_table(), lane_table(), twiddles()

    send = pl.pallas_call(sort_kernel, out_shape=shape(N_PY * CAP * 2, SLOTS), name="sort")(
        photons, halo_cells, halo_counts.reshape(-1, 1), owners
    )
    got = lax.all_to_all(
        send.reshape(N_PY, 2 * CAP, SLOTS), "py", 0, 0, tiled=True
    ).reshape(N_PY * CAP, 2, SLOTS)
    weights, cells = got[:, 0], got[:, 1].astype(jnp.int32)
    slot = jnp.arange(1, SLOTS + 1, dtype=jnp.int32)[None, :]
    counts = jnp.max(jnp.where(weights != 0, slot, 0), axis=1)

    send_a = pl.pallas_call(z_first_kernel, out_shape=shape(N_DEV * 2 * LB, 128), name="zfirst")(
        rows_density, *t_a
    )
    send_a, counts = lax.optimization_barrier((send_a, counts))
    got_a = exchange(send_a, 1)

    smem = pl.BlockSpec(memory_space=pltpu.SMEM)
    vmem = pl.BlockSpec(memory_space=pltpu.VMEM)
    send_bc = pl.pallas_call(
        paint_kernel,
        out_shape=shape(N_DEV * 4 * LB, 128),
        in_specs=[smem, smem, smem] + [vmem] * 7,
        scratch_shapes=[
            pltpu.VMEM((ROWS * 3, 128), F32),
            pltpu.VMEM((ROWS, NG), BF),
            pltpu.VMEM((ROWS, NG), BF),
        ],
        name="paint",
    )(weights, cells, counts, rows_density, *t_bd, *t_bs, *t_c)
    got_a, send_bc = lax.optimization_barrier((got_a, send_bc))
    got_bc = exchange(send_bc, 2)

    me = lax.axis_index(AXES)
    kz_b = jnp.where(me < 63, 129 + me, jnp.where(me < 126, me - 62, (me - 126) * (NG // 2)))
    win_a = window(me + 1)[None]
    win_bc = jnp.stack([window(kz_b), window(me + 64)])
    back_a = middle(got_a, 1, dev, lanes, tw, win_a)
    got_bc, back_a = lax.optimization_barrier((got_bc, back_a))
    home_a = exchange(back_a, 1)
    back_bc = middle(got_bc, 2, dev, lanes, tw, win_bc)
    home_a, back_bc = lax.optimization_barrier((home_a, back_bc))
    home_bc = exchange(back_bc, 2)
    fraction = pl.pallas_call(z_last_kernel, out_shape=shape(ROWS, NG), name="zlast")(
        home_a, home_bc, *t_a, *t_bd, *t_bs, *t_c
    )
    return fraction.reshape(CX, CY, NG)


def solution(mesh):
    placed = (
        P(("px", "py"), None),
        P(("px", "py"), None),
        P(("px", "py")),
        P(("px", "py"), None),
        P("px", "py", None),
    )
    return jax.shard_map(
        on_device, mesh=mesh, in_specs=placed, out_specs=P("px", "py", None), check_vma=False
    )
```

```python
import functools
import math

import jax
import jax.numpy as jnp
import ml_dtypes
import numpy as np
from jax import lax
from jax.experimental import pallas as pl
from jax.experimental.pallas import tpu as pltpu
from jax.sharding import PartitionSpec as P

NG = 384
SLOTS = 128
CAP = 4
RADIUS = 20
N_PX = 8
N_PY = 16
N_DEV = 128
CX = 48
CY = 24
ROWS = CX * CY
LB = ROWS // 128
PLANES = 3
WIDTH = 2 * LB
PITCH = PLANES * WIDTH
FIELDS = 4
AXES = ("px", "py")
BF = jnp.bfloat16
F32 = jnp.float32
NT = ((1,), (1,))
NN = ((1,), (0,))
TN = ((0,), (0,))
HALF_ROOT3 = math.sqrt(3.0) / 2.0

LANE_A, LANE_A2, LANE_B, LANE_Y = (
    g.reshape(-1) for g in np.meshgrid(range(3), range(3), range(16), range(8), indexing="ij")
)
LANE_CX = 16 * LANE_A + LANE_B
LANE_CY = 8 * LANE_A2 + LANE_Y


def split_np(table):
    high = table.astype(ml_dtypes.bfloat16)
    low = (table - high.astype(np.float64)).astype(ml_dtypes.bfloat16)
    return high, low


def z_table():
    z = np.arange(NG)
    table = np.zeros((3 * N_DEV, NG))
    for d in range(N_DEV):
        angle = 2.0 * np.pi * (((64 + d) * z) % NG) / NG
        table[d], table[N_DEV + d] = np.cos(angle), np.sin(angle)
    for d in range(N_DEV // 2):
        angle = 2.0 * np.pi * ((d * z) % NG) / NG
        table[2 * N_DEV + d], table[2 * N_DEV + 64 + d] = np.cos(angle), np.sin(angle)
    table[2 * N_DEV + 64] = 1.0 - 2.0 * (z % 2)
    return split_np(table)


def real_form(frac):
    angle = 2.0 * np.pi * (frac % 1.0)
    cos, sin = np.cos(angle), np.sin(angle)
    return np.block([[cos, sin], [-sin, cos]])


def device_table():
    s = np.arange(N_DEV)
    i, q = s // N_PY, s % N_PY
    return split_np(real_form(np.outer(i, i) / N_PX + np.outer(q, q) / N_PY))


def lane_table():
    m = np.arange(128)
    b, y = m // 8, m % 8
    return split_np(real_form(np.outer(b, b) / 16.0 + np.outer(y, y) / 8.0).T)


def twiddles():
    angle_x = 2.0 * np.pi * np.outer(np.arange(N_PX), LANE_CX) / NG
    angle_y = 2.0 * np.pi * np.outer(np.arange(N_PY), LANE_CY) / NG
    tw_x = np.stack([np.cos(angle_x), np.sin(angle_x)]).astype(np.float32)
    tw_y = np.stack([np.cos(angle_y), np.sin(angle_y)]).astype(np.float32)
    angle2 = 2.0 * np.pi * (LANE_B * LANE_A / 48.0 + LANE_Y * LANE_A2 / 24.0)
    tw2 = np.zeros((8, ROWS), np.float32)
    tw2[0], tw2[1] = np.cos(angle2), np.sin(angle2)
    return tw_x, tw_y, tw2


def window(kz):
    row = lax.broadcasted_iota(jnp.int32, (ROWS, 128), 0)
    lane = lax.broadcasted_iota(jnp.int32, (ROWS, 128), 1)
    u, k1 = row // N_DEV, row % N_DEV
    kx = k1 // N_PY + N_PX * (u // 3 + 3 * (lane // 8))
    ky = k1 % N_PY + N_PY * (u % 3 + 3 * (lane % 8))
    fx = jnp.where(kx < NG // 2, kx, kx - NG)
    fy = jnp.where(ky < NG // 2, ky, ky - NG)
    square = (fx * fx + fy * fy + kz * kz).astype(F32)
    radial = jnp.sqrt(square) * (2.0 * jnp.pi * RADIUS / NG)
    safe = jnp.where(radial > 0, radial, 1.0)
    value = 3.0 * (jnp.sin(safe) - safe * jnp.cos(safe)) / (safe * safe * safe)
    value = jnp.where(radial > 0, value, 1.0)
    both = (kz > 0) & (kz < NG // 2)
    return value * (jnp.where(both, 2.0, 1.0) / float(NG) ** 3)


def split(value):
    high = value.astype(BF)
    return high, (value - high.astype(F32)).astype(BF)


def dot(left, right, dims=NN):
    return lax.dot_general(left, right, (dims, ((), ())), preferred_element_type=F32)


def dot3(left, right, dims=NN):
    return (
        dot(left[0], right[0], dims) + dot(left[1], right[0], dims) + dot(left[0], right[1], dims)
    )


def sort_kernel(photons, cells, counts, owners, out):
    blocks = photons.shape[0]
    slots = N_PY * CAP
    target = owners[...]
    hot = jnp.where(
        lax.broadcasted_iota(jnp.int32, (N_PY, blocks), 0) == target, 1.0, 0.0
    )
    before = jnp.where(
        lax.broadcasted_iota(jnp.int32, (blocks, blocks), 0)
        < lax.broadcasted_iota(jnp.int32, (blocks, blocks), 1),
        1.0,
        0.0,
    )
    rank = jnp.sum(dot(hot.astype(BF), before.astype(BF)) * hot, axis=0, keepdims=True)
    place = target * CAP + rank.astype(jnp.int32)
    place_hot = jnp.where(
        lax.broadcasted_iota(jnp.int32, (slots, blocks), 0) == place, 1.0, 0.0
    )
    count = jnp.sum(place_hot * counts[...].astype(F32), axis=1, keepdims=True)
    live = lax.broadcasted_iota(jnp.int32, (slots, SLOTS), 1) < count.astype(jnp.int32)
    place_hot = place_hot.astype(BF)
    for half, value in enumerate((photons[...], cells[...].astype(F32))):
        rest, total = value, None
        for _ in range(3):
            first = rest.astype(BF)
            rest = rest - first.astype(F32)
            part = dot(place_hot, first)
            total = part if total is None else total + part
        out[pl.ds(half, slots, stride=2), :] = jnp.where(live, total, 0.0)


def z_density_kernel(density, t_high, t_low, out, few, high, low):
    for a in range(3):
        for a2 in range(3):
            block = density[a * 16 : (a + 1) * 16, a2 * 8 : (a2 + 1) * 8, :].reshape(128, NG)
            at = slice((a * 3 + a2) * 128, (a * 3 + a2 + 1) * 128)
            high[at, :], low[at, :] = split(block)
    for part in range(3):
        at = slice(part * N_DEV, (part + 1) * N_DEV)
        value = dot3((t_high[at, :], t_low[at, :]), (high[...], low[...]), NT)
        if part < 2:
            store_plane(out, part * LB, WIDTH, value)
        else:
            few[...] = value


def store_plane(out, start, pitch, value):
    for j in range(LB):
        rows = pl.ds(start + j, value.shape[0], stride=pitch)
        out[rows, :] = value[:, j * 128 : (j + 1) * 128]


def paint_kernel(weights, cells, counts, z_density, t_high, t_low, out, *scratch):
    fields, high, low = scratch[:FIELDS], scratch[FIELDS], scratch[FIELDS + 1]
    step = 8
    for field in fields:
        field[...] = jnp.zeros(field.shape, F32)
    lane = lax.broadcasted_iota(jnp.int32, (1, 128), 1)

    def block(index, carry):
        count = counts[index]
        for begin in range(0, SLOTS, step):

            @pl.when(count > begin)
            def _():
                for k in range(step):
                    cell = cells[index, begin + k]
                    value = weights[index, begin + k]
                    row = lax.shift_right_logical(cell, 7)
                    here = lane == (jnp.full((1, 128), cell, jnp.int32) & 127)
                    fields[k % FIELDS][pl.ds(row, 1), :] += jnp.where(here, value, 0.0)

        return carry

    lax.fori_loop(0, counts.shape[0], block, 0)
    for part in range(3):
        for a in range(3):
            for a2 in range(3):
                tiles = []
                for b in range(16):
                    row = (16 * a + b) * CY + 8 * a2
                    tile = fields[0][pl.ds(row * 3 + part, 8, stride=3), :]
                    for field in fields[1:]:
                        tile = tile + field[pl.ds(row * 3 + part, 8, stride=3), :]
                    tiles.append(tile)
                at = slice((a * 3 + a2) * 128, (a * 3 + a2 + 1) * 128)
                to = slice(part * 128, (part + 1) * 128)
                high[at, to], low[at, to] = split(jnp.concatenate(tiles, axis=0))
    source = (high[...], low[...])
    pitch = 2 * WIDTH
    for c in range(2):
        at = slice(c * N_DEV, (c + 1) * N_DEV)
        value = dot3((t_high[at, :], t_low[at, :]), source, NT)
        store_plane(out, WIDTH + c * LB, pitch, value)
    at = slice(2 * N_DEV, 3 * N_DEV)
    few = dot3((t_high[at, :], t_low[at, :]), source, NT)
    half = N_DEV // 2
    first = lax.broadcasted_iota(jnp.int32, (half, ROWS), 0) == 0
    dens_cos, dens_sin = z_density[:half, :], z_density[half:, :]
    phot_cos, phot_sin = few[:half], few[half:]
    store_plane(out, 0, pitch, jnp.where(first, phot_cos, dens_cos))
    store_plane(out, LB, pitch, jnp.where(first, dens_cos, dens_sin))
    store_plane(out, half * pitch, pitch, jnp.where(first, phot_sin, phot_cos))
    store_plane(out, half * pitch + LB, pitch, jnp.where(first, dens_sin, phot_sin))


def three(re, im, sign):
    t_re, t_im = re[1] + re[2], im[1] + im[2]
    d_re = (re[1] - re[2]) * (sign * HALF_ROOT3)
    d_im = (im[1] - im[2]) * (sign * HALF_ROOT3)
    m_re, m_im = re[0] - 0.5 * t_re, im[0] - 0.5 * t_im
    return (re[0] + t_re, m_re - d_im, m_re + d_im), (im[0] + t_im, m_im + d_re, m_im - d_re)


def nine(re, im, sign):
    for group in [(0, 1, 2), (3, 4, 5), (6, 7, 8), (0, 3, 6), (1, 4, 7), (2, 5, 8)]:
        new_re, new_im = three([re[g] for g in group], [im[g] for g in group], sign)
        for k, g in enumerate(group):
            re[g], im[g] = new_re[k], new_im[k]


def middle_kernel(planes, first_plane, got, *rest):
    if first_plane:
        rest = rest[1:]
    count = len(TABLE_SHAPES) + 1
    sources, out, rest = rest[:count], rest[count], rest[count + 1 :]
    tables, (tw1, work, r_high, r_low, l_high, l_low, back, sems) = rest[:count], rest[count:]
    dev_high, dev_low, lane_high, lane_low, tw_x, tw_y, tw2, win = tables
    copies = [
        pltpu.make_async_copy(source, table, sems.at[k])
        for k, (source, table) in enumerate(zip(sources, tables))
    ]
    for copy in copies:
        copy.start()
    pitch = planes * WIDTH
    for p in range(planes):
        for c in range(2):
            for j in range(LB):
                high, low = split(got[pl.ds((p * 2 + c) * LB + j, N_DEV, stride=pitch), :])
                at, to = slice(c * N_DEV, (c + 1) * N_DEV), slice(j * 128, (j + 1) * 128)
                r_high[p, at, to] = high
                r_low[p, at, to] = low
    for copy in copies:
        copy.wait()
    for k in range(N_PX):
        cos_x, sin_x = tw_x[0, k : k + 1, :], tw_x[1, k : k + 1, :]
        cos_y, sin_y = tw_y[0], tw_y[1]
        at = slice(k * N_PY, (k + 1) * N_PY)
        tw1[0, at, :] = cos_x * cos_y - sin_x * sin_y
        tw1[1, at, :] = sin_x * cos_y + cos_x * sin_y

    def plane(p, carry):
        dev = (dev_high[...], dev_low[...])
        for a in range(3):
            at = slice(a * NG, (a + 1) * NG)
            work[:, at] = dot3(dev, (r_high[p, :, at], r_low[p, :, at]))

        def forward(block, inner):
            rows = pl.ds(pl.multiple_of(block * 16, 16), 16)
            rows_im = pl.ds(pl.multiple_of(block * 16 + N_DEV, 16), 16)
            re, im = [], []
            for j in range(LB):
                at = slice(j * 128, (j + 1) * 128)
                cos, sin = tw1[0, rows, at], tw1[1, rows, at]
                x, y = work[rows, at], work[rows_im, at]
                re.append(x * cos + y * sin)
                im.append(y * cos - x * sin)
            nine(re, im, -1.0)
            for j in range(LB):
                at = slice(j * 128, (j + 1) * 128)
                cos, sin = tw2[0:1, at], tw2[1:2, at]
                to = pl.ds(pl.multiple_of(block * 16 + j * N_DEV, 16), 16)
                l_high[to, :128], l_low[to, :128] = split(re[j] * cos + im[j] * sin)
                l_high[to, 128:], l_low[to, 128:] = split(im[j] * cos - re[j] * sin)
            return inner

        lax.fori_loop(0, N_DEV // 16, forward, 0)
        mat = (lane_high[...], lane_low[...])
        for k in range(3):
            at = slice(k * NG, (k + 1) * NG)
            value = dot3((l_high[at, :], l_low[at, :]), mat)
            w = win[p, at, :]
            l_high[at, :128], l_low[at, :128] = split(value[:, :128] * w)
            l_high[at, 128:], l_low[at, 128:] = split(value[:, 128:] * w)
            back[at, :] = dot3((l_high[at, :], l_low[at, :]), mat, NT)

        def backward(block, inner):
            rows = pl.ds(pl.multiple_of(block * 16, 16), 16)
            rows_im = pl.ds(pl.multiple_of(block * 16 + N_DEV, 16), 16)
            re, im = [], []
            for j in range(LB):
                at = slice(j * 128, (j + 1) * 128)
                cos, sin = tw2[0:1, at], tw2[1:2, at]
                of = pl.ds(pl.multiple_of(block * 16 + j * N_DEV, 16), 16)
                x, y = back[of, :128], back[of, 128:]
                re.append(x * cos - y * sin)
                im.append(y * cos + x * sin)
            nine(re, im, 1.0)
            for j in range(LB):
                at = slice(j * 128, (j + 1) * 128)
                cos, sin = tw1[0, rows, at], tw1[1, rows, at]
                r_high[p, rows, at], r_low[p, rows, at] = split(re[j] * cos - im[j] * sin)
                r_high[p, rows_im, at], r_low[p, rows_im, at] = split(im[j] * cos + re[j] * sin)
            return inner

        lax.fori_loop(0, N_DEV // 16, backward, 0)
        for a in range(3):
            at = slice(a * NG, (a + 1) * NG)
            value = dot3(dev, (r_high[p, :, at], r_low[p, :, at]), TN)
            for c in range(2):
                for j in range(3):
                    start = (first_plane + p) * WIDTH + c * LB + a * 3 + j
                    out[pl.ds(start, N_DEV, stride=PITCH), :] = value[
                        c * N_DEV : (c + 1) * N_DEV, j * 128 : (j + 1) * 128
                    ]
        return carry

    lax.fori_loop(0, planes, plane, 0)


def z_last_kernel(got, t_high, t_low, out):
    a = pl.program_id(0)
    half = N_DEV // 2
    first = lax.broadcasted_iota(jnp.int32, (half, 128), 0) == 0
    dens, phot = [], []
    for a2 in range(3):

        def load(plane, c, begin=0, count=N_DEV):
            start = begin * PITCH + (plane * 2 + c) * LB + a * 3 + a2
            return got[pl.ds(start, count, stride=PITCH), :]

        re_low, im_low = load(1, 0, 0, half), load(1, 1, 0, half)
        re_top, im_top = load(1, 0, half, half), load(1, 1, half, half)
        dens.append(
            jnp.concatenate(
                [
                    load(0, 0),
                    load(0, 1),
                    jnp.where(first, im_low, re_low),
                    jnp.where(first, im_top, im_low),
                ],
                axis=0,
            )
        )
        phot.append(
            jnp.concatenate(
                [
                    load(2, 0),
                    load(2, 1),
                    jnp.where(first, re_low, re_top),
                    jnp.where(first, re_top, im_top),
                ],
                axis=0,
            )
        )
    table = (t_high[...], t_low[...])
    smooth_d = dot3(split(jnp.concatenate(dens, axis=1)), table, TN)
    smooth_p = dot3(split(jnp.concatenate(phot, axis=1)), table, TN)
    value = jnp.clip(smooth_p / jnp.maximum(smooth_d, 0.5), 0.0, 1.0)
    for a2 in range(3):
        out[:, a2 * 8 : (a2 + 1) * 8, :] = value[a2 * 128 : (a2 + 1) * 128].reshape(16, 8, NG)


TABLE_SHAPES = [((256, 256), BF)] * 4 + [
    ((2, N_PX, ROWS), F32),
    ((2, N_PY, ROWS), F32),
    ((8, ROWS), F32),
]


def placed_in(space, *arrays):
    return [pltpu.with_memory_space_constraint(jnp.asarray(a), space) for a in arrays]


def limit(mib):
    return pltpu.CompilerParams(vmem_limit_bytes=mib * 2**20)


def exchange(rows):
    send = rows.reshape(N_DEV, 1, rows.size // N_DEV)
    return lax.all_to_all(send, AXES, 0, 0, tiled=True).reshape(rows.shape)


def middle(got, planes, first_plane, tables, win, begun=None):
    anywhere = pl.BlockSpec(memory_space=pl.ANY)
    vmem = pl.BlockSpec(memory_space=pltpu.VMEM)
    begun = [] if begun is None else [begun]
    shapes = TABLE_SHAPES + [(win.shape, F32)]
    return pl.pallas_call(
        functools.partial(middle_kernel, planes, first_plane),
        out_shape=pltpu.VMEM((N_DEV * PITCH, 128), F32),
        in_specs=[vmem] * (1 + len(begun)) + [anywhere] * len(shapes),
        input_output_aliases={1: 0} if begun else {},
        scratch_shapes=[pltpu.VMEM(*shape) for shape in shapes]
        + [
            pltpu.VMEM((2, N_DEV, ROWS), F32),
            pltpu.VMEM((2 * N_DEV, ROWS), F32),
            pltpu.VMEM((planes, 2 * N_DEV, ROWS), BF),
            pltpu.VMEM((planes, 2 * N_DEV, ROWS), BF),
            pltpu.VMEM((ROWS, 256), BF),
            pltpu.VMEM((ROWS, 256), BF),
            pltpu.VMEM((ROWS, 256), F32),
            pltpu.SemaphoreType.DMA((len(shapes),)),
        ],
        compiler_params=limit(20),
        name=f"middle{planes}",
    )(*placed_in(pltpu.VMEM, got, *begun), *placed_in(pltpu.HBM, *tables, win))


def on_device(photons, halo_cells, halo_counts, owners, density):
    table = z_table()
    tables = (*device_table(), *lane_table(), *twiddles())

    send = pl.pallas_call(
        sort_kernel,
        out_shape=jax.ShapeDtypeStruct((N_PY * CAP * 2, SLOTS), F32),
        name="sort",
    )(photons, halo_cells, halo_counts.reshape(1, -1), owners.reshape(1, -1))
    halos = lax.all_to_all(send.reshape(N_PY, 2 * CAP, SLOTS), "py", 0, 0, tiled=True)

    send_a, few = pl.pallas_call(
        z_density_kernel,
        out_shape=(
            jax.ShapeDtypeStruct((N_DEV * WIDTH, 128), F32),
            jax.ShapeDtypeStruct((N_DEV, ROWS), F32),
        ),
        scratch_shapes=[pltpu.VMEM((ROWS, NG), BF), pltpu.VMEM((ROWS, NG), BF)],
        name="zdensity",
    )(density, *table)
    send_a, halos = lax.optimization_barrier((send_a, halos))
    got_a = exchange(send_a)

    halos = halos.reshape(N_PY * CAP, 2, SLOTS)
    weights, cells = halos[:, 0], halos[:, 1].astype(jnp.int32)
    slot = jnp.arange(1, SLOTS + 1, dtype=jnp.int32)[None, :]
    counts = jnp.max(jnp.where(weights != 0, slot, 0), axis=1)
    smem = pl.BlockSpec(memory_space=pltpu.SMEM)
    vmem = pl.BlockSpec(memory_space=pltpu.VMEM)
    send_bc = pl.pallas_call(
        paint_kernel,
        out_shape=jax.ShapeDtypeStruct((N_DEV * 2 * WIDTH, 128), F32),
        in_specs=[smem, smem, smem, vmem, vmem, vmem],
        scratch_shapes=[pltpu.VMEM((ROWS * 3, 128), F32)] * FIELDS
        + [pltpu.VMEM((ROWS, NG), BF), pltpu.VMEM((ROWS, NG), BF)],
        name="paint",
    )(weights, cells, counts, few, *table)
    got_a, send_bc = lax.optimization_barrier((got_a, send_bc))
    got_bc = exchange(send_bc)

    me = lax.axis_index(AXES)
    half = N_DEV // 2
    low = jnp.where(me % half == 0, (me // half) * (NG // 2), me % half)
    win_a = window(me + 64)
    win_bc = jnp.stack([window(low), win_a])
    back = middle(got_a, 1, 0, tables, win_a[None])
    back = middle(got_bc, 2, 1, tables, win_bc, back)
    got = exchange(back)
    whole = pl.BlockSpec((N_DEV * PITCH, 128), lambda i: (0, 0))
    whole_t = pl.BlockSpec((3 * N_DEV, NG), lambda i: (0, 0))
    return pl.pallas_call(
        z_last_kernel,
        grid=(3,),
        in_specs=[whole, whole_t, whole_t],
        out_specs=pl.BlockSpec((16, CY, NG), lambda i: (i, 0, 0)),
        out_shape=jax.ShapeDtypeStruct((CX, CY, NG), F32),
        compiler_params=limit(16),
        name="zlast",
    )(*placed_in(pltpu.VMEM, got, *table))


def solution(mesh):
    placed = (
        P(("px", "py"), None),
        P(("px", "py"), None),
        P(("px", "py")),
        P(("px", "py"), None),
        P("px", "py", None),
    )
    return jax.shard_map(
        on_device, mesh=mesh, in_specs=placed, out_specs=P("px", "py", None), check_vma=False
    )
```

```python
import functools
import math

import jax
import jax.numpy as jnp
import ml_dtypes
import numpy as np
from jax import lax
from jax.experimental import pallas as pl
from jax.experimental.pallas import tpu as pltpu
from jax.sharding import PartitionSpec as P

NG = 384
SLOTS = 128
CAP = 4
RADIUS = 20
N_PX = 8
N_PY = 16
N_DEV = 128
CX = 48
CY = 24
ROWS = CX * CY
LB = ROWS // 128
PLANES = 3
WIDTH = 2 * LB
PITCH = PLANES * WIDTH
FIELDS = 4
AXES = ("px", "py")
BF = jnp.bfloat16
F32 = jnp.float32
NT = ((1,), (1,))
NN = ((1,), (0,))
TN = ((0,), (0,))
HALF_ROOT3 = math.sqrt(3.0) / 2.0

LANE_A, LANE_A2, LANE_B, LANE_Y = (
    g.reshape(-1) for g in np.meshgrid(range(3), range(3), range(16), range(8), indexing="ij")
)
LANE_CX = 16 * LANE_A + LANE_B
LANE_CY = 8 * LANE_A2 + LANE_Y


def split_np(table):
    high = table.astype(ml_dtypes.bfloat16)
    low = (table - high.astype(np.float64)).astype(ml_dtypes.bfloat16)
    return high, low


def z_table():
    z = np.arange(NG)
    table = np.zeros((3 * N_DEV, NG))
    for d in range(N_DEV):
        angle = 2.0 * np.pi * (((64 + d) * z) % NG) / NG
        table[d], table[N_DEV + d] = np.cos(angle), np.sin(angle)
    for d in range(N_DEV // 2):
        angle = 2.0 * np.pi * ((d * z) % NG) / NG
        table[2 * N_DEV + d], table[2 * N_DEV + 64 + d] = np.cos(angle), np.sin(angle)
    table[2 * N_DEV + 64] = 1.0 - 2.0 * (z % 2)
    return split_np(table)


def real_form(frac):
    angle = 2.0 * np.pi * (frac % 1.0)
    cos, sin = np.cos(angle), np.sin(angle)
    return np.block([[cos, sin], [-sin, cos]])


def device_table():
    s = np.arange(N_DEV)
    i, q = s // N_PY, s % N_PY
    return split_np(real_form(np.outer(i, i) / N_PX + np.outer(q, q) / N_PY))


def lane_table():
    m = np.arange(128)
    b, y = m // 8, m % 8
    return split_np(real_form(np.outer(b, b) / 16.0 + np.outer(y, y) / 8.0).T)


def twiddles():
    angle_x = 2.0 * np.pi * np.outer(np.arange(N_PX), LANE_CX) / NG
    angle_y = 2.0 * np.pi * np.outer(np.arange(N_PY), LANE_CY) / NG
    tw_x = np.stack([np.cos(angle_x), np.sin(angle_x)]).astype(np.float32)
    tw_y = np.stack([np.cos(angle_y), np.sin(angle_y)]).astype(np.float32)
    angle2 = 2.0 * np.pi * (LANE_B * LANE_A / 48.0 + LANE_Y * LANE_A2 / 24.0)
    tw2 = np.zeros((8, ROWS), np.float32)
    tw2[0], tw2[1] = np.cos(angle2), np.sin(angle2)
    return tw_x, tw_y, tw2


def window(kz):
    row = lax.broadcasted_iota(jnp.int32, (ROWS, 128), 0)
    lane = lax.broadcasted_iota(jnp.int32, (ROWS, 128), 1)
    u, k1 = row // N_DEV, row % N_DEV
    kx = k1 // N_PY + N_PX * (u // 3 + 3 * (lane // 8))
    ky = k1 % N_PY + N_PY * (u % 3 + 3 * (lane % 8))
    fx = jnp.where(kx < NG // 2, kx, kx - NG)
    fy = jnp.where(ky < NG // 2, ky, ky - NG)
    square = (fx * fx + fy * fy + kz * kz).astype(F32)
    radial = jnp.sqrt(square) * (2.0 * jnp.pi * RADIUS / NG)
    safe = jnp.where(radial > 0, radial, 1.0)
    value = 3.0 * (jnp.sin(safe) - safe * jnp.cos(safe)) / (safe * safe * safe)
    value = jnp.where(radial > 0, value, 1.0)
    both = (kz > 0) & (kz < NG // 2)
    return value * (jnp.where(both, 2.0, 1.0) / float(NG) ** 3)


def split(value):
    high = value.astype(BF)
    return high, (value - high.astype(F32)).astype(BF)


def dot(left, right, dims=NN):
    return lax.dot_general(left, right, (dims, ((), ())), preferred_element_type=F32)


def dot3(left, right, dims=NN):
    (left_dim,), (right_dim,) = dims
    return dot(
        jnp.concatenate([left[0], left[1], left[0]], axis=left_dim),
        jnp.concatenate([right[0], right[0], right[1]], axis=right_dim),
        dims,
    )


def sort_kernel(photons, cells, counts, owners, out):
    blocks = photons.shape[0]
    slots = N_PY * CAP
    target = owners[...]
    hot = jnp.where(
        lax.broadcasted_iota(jnp.int32, (N_PY, blocks), 0) == target, 1.0, 0.0
    )
    before = jnp.where(
        lax.broadcasted_iota(jnp.int32, (blocks, blocks), 0)
        < lax.broadcasted_iota(jnp.int32, (blocks, blocks), 1),
        1.0,
        0.0,
    )
    rank = jnp.sum(dot(hot.astype(BF), before.astype(BF)) * hot, axis=0, keepdims=True)
    place = target * CAP + rank.astype(jnp.int32)
    place_hot = jnp.where(
        lax.broadcasted_iota(jnp.int32, (slots, blocks), 0) == place, 1.0, 0.0
    )
    count = jnp.sum(place_hot * counts[...].astype(F32), axis=1, keepdims=True)
    live = lax.broadcasted_iota(jnp.int32, (slots, SLOTS), 1) < count.astype(jnp.int32)
    place_hot = place_hot.astype(BF)
    for half, value in enumerate((photons[...], cells[...].astype(F32))):
        rest, total = value, None
        for _ in range(3):
            first = rest.astype(BF)
            rest = rest - first.astype(F32)
            part = dot(place_hot, first)
            total = part if total is None else total + part
        out[pl.ds(half, slots, stride=2), :] = jnp.where(live, total, 0.0)


def z_density_kernel(density, t_high, t_low, out, few, high, low):
    for a in range(3):
        for a2 in range(3):
            block = density[a * 16 : (a + 1) * 16, a2 * 8 : (a2 + 1) * 8, :].reshape(128, NG)
            at = slice((a * 3 + a2) * 128, (a * 3 + a2 + 1) * 128)
            high[at, :], low[at, :] = split(block)
    for a in range(3):
        at = slice(a * NG, (a + 1) * NG)
        value = dot3((t_high[...], t_low[...]), (high[at, :], low[at, :]), NT)
        for c in range(2):
            store_plane(out, c * LB + 3 * a, WIDTH, value[c * N_DEV : (c + 1) * N_DEV])
        few[:, at] = value[2 * N_DEV :]


def store_plane(out, start, pitch, value):
    for j in range(value.shape[1] // 128):
        rows = pl.ds(start + j, value.shape[0], stride=pitch)
        out[rows, :] = value[:, j * 128 : (j + 1) * 128]


def paint_kernel(weights, cells, counts, z_density, t_high, t_low, out, *scratch):
    fields, high, low = scratch[:FIELDS], scratch[FIELDS], scratch[FIELDS + 1]
    for field in fields:
        field[...] = jnp.zeros(field.shape, F32)
    lane = lax.broadcasted_iota(jnp.int32, (1, 128), 1)

    def block(index, carry):
        count = counts[index]

        def some(begin, step):
            for k in range(begin, begin + step):
                cell = cells[index, k]
                value = weights[index, k]
                row = lax.shift_right_logical(cell, 7)
                here = lane == (jnp.full((1, 128), cell, jnp.int32) & 127)
                fields[k % FIELDS][pl.ds(row, 1), :] += jnp.where(here, value, 0.0)

        def halves(begin, size):
            @pl.when(count > begin)
            def _():
                if size == 16:
                    some(begin, size)
                else:
                    halves(begin, size // 2)
                    halves(begin + size // 2, size // 2)

        halves(0, SLOTS)
        return carry

    lax.fori_loop(0, counts.shape[0], block, 0)
    for part in range(3):
        for a in range(3):
            for a2 in range(3):
                tiles = []
                for b in range(16):
                    row = (16 * a + b) * CY + 8 * a2
                    tile = fields[0][pl.ds(row * 3 + part, 8, stride=3), :]
                    for field in fields[1:]:
                        tile = tile + field[pl.ds(row * 3 + part, 8, stride=3), :]
                    tiles.append(tile)
                at = slice((a * 3 + a2) * 128, (a * 3 + a2 + 1) * 128)
                to = slice(part * 128, (part + 1) * 128)
                high[at, to], low[at, to] = split(jnp.concatenate(tiles, axis=0))
    pitch = 2 * WIDTH
    half = N_DEV // 2
    first = lax.broadcasted_iota(jnp.int32, (half, NG), 0) == 0
    for a in range(3):
        at = slice(a * NG, (a + 1) * NG)
        value = dot3((t_high[...], t_low[...]), (high[at, :], low[at, :]), NT)
        for c in range(2):
            plane = value[c * N_DEV : (c + 1) * N_DEV]
            store_plane(out, WIDTH + c * LB + 3 * a, pitch, plane)
        dens_cos, dens_sin = z_density[:half, at], z_density[half:, at]
        phot_cos, phot_sin = value[2 * N_DEV : 2 * N_DEV + half], value[2 * N_DEV + half :]
        low_rows, top_rows = 3 * a, half * pitch + 3 * a
        store_plane(out, low_rows, pitch, jnp.where(first, phot_cos, dens_cos))
        store_plane(out, low_rows + LB, pitch, jnp.where(first, dens_cos, dens_sin))
        store_plane(out, top_rows, pitch, jnp.where(first, phot_sin, phot_cos))
        store_plane(out, top_rows + LB, pitch, jnp.where(first, dens_sin, phot_sin))


def three(re, im, sign):
    t_re, t_im = re[1] + re[2], im[1] + im[2]
    d_re = (re[1] - re[2]) * (sign * HALF_ROOT3)
    d_im = (im[1] - im[2]) * (sign * HALF_ROOT3)
    m_re, m_im = re[0] - 0.5 * t_re, im[0] - 0.5 * t_im
    return (re[0] + t_re, m_re - d_im, m_re + d_im), (im[0] + t_im, m_im + d_re, m_im - d_re)


def nine(re, im, sign):
    for group in [(0, 1, 2), (3, 4, 5), (6, 7, 8), (0, 3, 6), (1, 4, 7), (2, 5, 8)]:
        new_re, new_im = three([re[g] for g in group], [im[g] for g in group], sign)
        for k, g in enumerate(group):
            re[g], im[g] = new_re[k], new_im[k]


def middle_kernel(planes, got, *rest):
    count = len(TABLE_SHAPES) + (2 if planes == 2 else 1)
    sources, out, rest = rest[:count], rest[count], rest[count + 1 :]
    tables, (tw1, work, r_high, r_low, l_high, l_low, back, sems) = rest[:count], rest[count:]
    dev_high, dev_low, lane_high, lane_low, tw_x, tw_y, tw2, win = tables[:8]
    copies = [
        pltpu.make_async_copy(source, table, sems.at[k])
        for k, (source, table) in enumerate(zip(sources, tables))
    ]
    for copy in copies:
        copy.start()
    first_plane, out_pitch = (1, PITCH) if planes == 2 else (0, WIDTH)
    pitch = planes * WIDTH
    for p in range(planes):
        for c in range(2):
            for j in range(LB):
                high, low = split(got[pl.ds((p * 2 + c) * LB + j, N_DEV, stride=pitch), :])
                at, to = slice(c * N_DEV, (c + 1) * N_DEV), slice(j * 128, (j + 1) * 128)
                r_high[p, at, to] = high
                r_low[p, at, to] = low
    for copy in copies[:7]:
        copy.wait()
    for k in range(N_PX):
        cos_x, sin_x = tw_x[0, k : k + 1, :], tw_x[1, k : k + 1, :]
        cos_y, sin_y = tw_y[0], tw_y[1]
        at = slice(k * N_PY, (k + 1) * N_PY)
        tw1[0, at, :] = cos_x * cos_y - sin_x * sin_y
        tw1[1, at, :] = sin_x * cos_y + cos_x * sin_y

    def plane(p, carry):
        dev = (dev_high[...], dev_low[...])
        for a in range(3):
            at = slice(a * NG, (a + 1) * NG)
            work[:, at] = dot3(dev, (r_high[p, :, at], r_low[p, :, at]))

        def forward(block, inner):
            rows = pl.ds(pl.multiple_of(block * 16, 16), 16)
            rows_im = pl.ds(pl.multiple_of(block * 16 + N_DEV, 16), 16)
            re, im = [], []
            for j in range(LB):
                at = slice(j * 128, (j + 1) * 128)
                cos, sin = tw1[0, rows, at], tw1[1, rows, at]
                x, y = work[rows, at], work[rows_im, at]
                re.append(x * cos + y * sin)
                im.append(y * cos - x * sin)
            nine(re, im, -1.0)
            for j in range(LB):
                at = slice(j * 128, (j + 1) * 128)
                cos, sin = tw2[0:1, at], tw2[1:2, at]
                to = pl.ds(pl.multiple_of(block * 16 + j * N_DEV, 16), 16)
                l_high[to, :128], l_low[to, :128] = split(re[j] * cos + im[j] * sin)
                l_high[to, 128:], l_low[to, 128:] = split(im[j] * cos - re[j] * sin)
            return inner

        lax.fori_loop(0, N_DEV // 16, forward, 0)

        @pl.when(p == 0)
        def _():
            for copy in copies[7:]:
                copy.wait()

        mat = (lane_high[...], lane_low[...])
        for k in range(3):
            at = slice(k * NG, (k + 1) * NG)
            value = dot3((l_high[at, :], l_low[at, :]), mat)
            w = win[p, at, :]
            l_high[at, :128], l_low[at, :128] = split(value[:, :128] * w)
            l_high[at, 128:], l_low[at, 128:] = split(value[:, 128:] * w)
            back[at, :] = dot3((l_high[at, :], l_low[at, :]), mat, NT)

        def backward(block, inner):
            rows = pl.ds(pl.multiple_of(block * 16, 16), 16)
            rows_im = pl.ds(pl.multiple_of(block * 16 + N_DEV, 16), 16)
            re, im = [], []
            for j in range(LB):
                at = slice(j * 128, (j + 1) * 128)
                cos, sin = tw2[0:1, at], tw2[1:2, at]
                of = pl.ds(pl.multiple_of(block * 16 + j * N_DEV, 16), 16)
                x, y = back[of, :128], back[of, 128:]
                re.append(x * cos - y * sin)
                im.append(y * cos + x * sin)
            nine(re, im, 1.0)
            for j in range(LB):
                at = slice(j * 128, (j + 1) * 128)
                cos, sin = tw1[0, rows, at], tw1[1, rows, at]
                r_high[p, rows, at], r_low[p, rows, at] = split(re[j] * cos - im[j] * sin)
                r_high[p, rows_im, at], r_low[p, rows_im, at] = split(im[j] * cos + re[j] * sin)
            return inner

        lax.fori_loop(0, N_DEV // 16, backward, 0)
        for a in range(3):
            at = slice(a * NG, (a + 1) * NG)
            value = dot3(dev, (r_high[p, :, at], r_low[p, :, at]), TN)
            for c in range(2):
                for j in range(3):
                    start = (first_plane + p) * WIDTH + c * LB + a * 3 + j
                    out[pl.ds(start, N_DEV, stride=out_pitch), :] = value[
                        c * N_DEV : (c + 1) * N_DEV, j * 128 : (j + 1) * 128
                    ]
        return carry

    lax.fori_loop(0, planes, plane, 0)
    if planes == 2:
        for j in range(WIDTH):
            out[pl.ds(j, N_DEV, stride=PITCH), :] = tables[8][pl.ds(j, N_DEV, stride=WIDTH), :]


def z_last_kernel(got, t_high, t_low, out):
    a = pl.program_id(0)
    half = N_DEV // 2
    first = lax.broadcasted_iota(jnp.int32, (half, 128), 0) == 0
    dens, phot = [], []
    for a2 in range(3):

        def load(plane, c, begin=0, count=N_DEV):
            start = begin * PITCH + (plane * 2 + c) * LB + a * 3 + a2
            return got[pl.ds(start, count, stride=PITCH), :]

        re_low, im_low = load(1, 0, 0, half), load(1, 1, 0, half)
        re_top, im_top = load(1, 0, half, half), load(1, 1, half, half)
        dens.append(
            jnp.concatenate(
                [
                    load(0, 0),
                    load(0, 1),
                    jnp.where(first, im_low, re_low),
                    jnp.where(first, im_top, im_low),
                ],
                axis=0,
            )
        )
        phot.append(
            jnp.concatenate(
                [
                    load(2, 0),
                    load(2, 1),
                    jnp.where(first, re_low, re_top),
                    jnp.where(first, re_top, im_top),
                ],
                axis=0,
            )
        )
    table = (t_high[...], t_low[...])
    smooth_d = dot3(split(jnp.concatenate(dens, axis=1)), table, TN)
    smooth_p = dot3(split(jnp.concatenate(phot, axis=1)), table, TN)
    value = jnp.clip(smooth_p / jnp.maximum(smooth_d, 0.5), 0.0, 1.0)
    for a2 in range(3):
        out[:, a2 * 8 : (a2 + 1) * 8, :] = value[a2 * 128 : (a2 + 1) * 128].reshape(16, 8, NG)


TABLE_SHAPES = [((256, 256), BF)] * 4 + [
    ((2, N_PX, ROWS), F32),
    ((2, N_PY, ROWS), F32),
    ((8, ROWS), F32),
]


def placed_in(space, *arrays):
    return [pltpu.with_memory_space_constraint(jnp.asarray(a), space) for a in arrays]


def limit(mib):
    return pltpu.CompilerParams(vmem_limit_bytes=mib * 2**20)


def exchange(rows):
    send = rows.reshape(N_DEV, 1, rows.size // N_DEV)
    return lax.all_to_all(send, AXES, 0, 0, tiled=True).reshape(rows.shape)


def middle(got, planes, sources):
    shapes = TABLE_SHAPES + [(source.shape, F32) for source in sources[len(TABLE_SHAPES) :]]
    if planes == 2:
        out_shape = pltpu.VMEM((N_DEV * PITCH, 128), F32)
    else:
        out_shape = jax.ShapeDtypeStruct((N_DEV * WIDTH, 128), F32)
    return pl.pallas_call(
        functools.partial(middle_kernel, planes),
        out_shape=out_shape,
        in_specs=[pl.BlockSpec(memory_space=pltpu.VMEM)]
        + [pl.BlockSpec(memory_space=pl.ANY)] * len(shapes),
        scratch_shapes=[pltpu.VMEM(*shape) for shape in shapes]
        + [
            pltpu.VMEM((2, N_DEV, ROWS), F32),
            pltpu.VMEM((2 * N_DEV, ROWS), F32),
            pltpu.VMEM((planes, 2 * N_DEV, ROWS), BF),
            pltpu.VMEM((planes, 2 * N_DEV, ROWS), BF),
            pltpu.VMEM((ROWS, 256), BF),
            pltpu.VMEM((ROWS, 256), BF),
            pltpu.VMEM((ROWS, 256), F32),
            pltpu.SemaphoreType.DMA((len(shapes),)),
        ],
        compiler_params=limit(20),
        name=f"middle{planes}",
    )(*placed_in(pltpu.VMEM, got), *placed_in(pltpu.HBM, *sources))


def on_device(photons, halo_cells, halo_counts, owners, density):
    table = z_table()
    tables = (*device_table(), *lane_table(), *twiddles())

    send = pl.pallas_call(
        sort_kernel,
        out_shape=jax.ShapeDtypeStruct((N_PY * CAP * 2, SLOTS), F32),
        name="sort",
    )(photons, halo_cells, halo_counts.reshape(1, -1), owners.reshape(1, -1))
    halos = lax.all_to_all(send.reshape(N_PY, 2 * CAP, SLOTS), "py", 0, 0, tiled=True)

    send_a, few = pl.pallas_call(
        z_density_kernel,
        out_shape=(
            jax.ShapeDtypeStruct((N_DEV * WIDTH, 128), F32),
            jax.ShapeDtypeStruct((N_DEV, ROWS), F32),
        ),
        scratch_shapes=[pltpu.VMEM((ROWS, NG), BF), pltpu.VMEM((ROWS, NG), BF)],
        name="zdensity",
    )(density, *table)
    send_a, halos = lax.optimization_barrier((send_a, halos))
    got_a = exchange(send_a)

    halos = halos.reshape(N_PY * CAP, 2, SLOTS)
    weights, cells = halos[:, 0], halos[:, 1].astype(jnp.int32)
    slot = jnp.arange(1, SLOTS + 1, dtype=jnp.int32)[None, :]
    counts = jnp.max(jnp.where(weights != 0, slot, 0), axis=1)
    smem = pl.BlockSpec(memory_space=pltpu.SMEM)
    vmem = pl.BlockSpec(memory_space=pltpu.VMEM)
    send_bc = pl.pallas_call(
        paint_kernel,
        out_shape=jax.ShapeDtypeStruct((N_DEV * 2 * WIDTH, 128), F32),
        in_specs=[smem, smem, smem, vmem, vmem, vmem],
        scratch_shapes=[pltpu.VMEM((ROWS * 3, 128), F32)] * FIELDS
        + [pltpu.VMEM((ROWS, NG), BF), pltpu.VMEM((ROWS, NG), BF)],
        name="paint",
    )(weights, cells, counts, few, *table)
    got_bc = exchange(send_bc)

    me = lax.axis_index(AXES)
    half = N_DEV // 2
    low = jnp.where(me % half == 0, (me // half) * (NG // 2), me % half)
    win_a = window(me + 64)
    win_bc = jnp.stack([window(low), win_a])
    back_a = middle(got_a, 1, (*tables, win_a[None]))
    back = middle(got_bc, 2, (*tables, win_bc, back_a))
    got = exchange(back)
    whole = pl.BlockSpec((N_DEV * PITCH, 128), lambda i: (0, 0))
    whole_t = pl.BlockSpec((3 * N_DEV, NG), lambda i: (0, 0))
    return pl.pallas_call(
        z_last_kernel,
        grid=(3,),
        in_specs=[whole, whole_t, whole_t],
        out_specs=pl.BlockSpec((16, CY, NG), lambda i: (i, 0, 0)),
        out_shape=jax.ShapeDtypeStruct((CX, CY, NG), F32),
        compiler_params=limit(16),
        name="zlast",
    )(*placed_in(pltpu.VMEM, got, *table))


def solution(mesh):
    placed = (
        P(("px", "py"), None),
        P(("px", "py"), None),
        P(("px", "py")),
        P(("px", "py"), None),
        P("px", "py", None),
    )
    return jax.shard_map(
        on_device, mesh=mesh, in_specs=placed, out_specs=P("px", "py", None), check_vma=False
    )
```

```python
import functools
import math

import jax
import jax.numpy as jnp
import ml_dtypes
import numpy as np
from jax import lax
from jax.experimental import pallas as pl
from jax.experimental.pallas import tpu as pltpu
from jax.sharding import PartitionSpec as P

NG = 384
SLOTS = 128
CAP = 4
RADIUS = 20
N_PX = 8
N_PY = 16
N_DEV = 128
CX = 48
CY = 24
ROWS = CX * CY
LB = ROWS // 128
PLANES = 3
WIDTH = 2 * LB
PITCH = PLANES * WIDTH
FIELDS = 4
AXES = ("px", "py")
BF = jnp.bfloat16
F32 = jnp.float32
NT = ((1,), (1,))
NN = ((1,), (0,))
TN = ((0,), (0,))
HALF_ROOT3 = math.sqrt(3.0) / 2.0

LANE_A, LANE_A2, LANE_B, LANE_Y = (
    g.reshape(-1) for g in np.meshgrid(range(3), range(3), range(16), range(8), indexing="ij")
)
LANE_CX = 16 * LANE_A + LANE_B
LANE_CY = 8 * LANE_A2 + LANE_Y


def split_np(table):
    high = table.astype(ml_dtypes.bfloat16)
    low = (table - high.astype(np.float64)).astype(ml_dtypes.bfloat16)
    return high, low


def z_table():
    z = np.arange(NG)
    table = np.zeros((3 * N_DEV, NG))
    for d in range(N_DEV):
        angle = 2.0 * np.pi * (((64 + d) * z) % NG) / NG
        table[d], table[N_DEV + d] = np.cos(angle), np.sin(angle)
    for d in range(N_DEV // 2):
        angle = 2.0 * np.pi * ((d * z) % NG) / NG
        table[2 * N_DEV + d], table[2 * N_DEV + 64 + d] = np.cos(angle), np.sin(angle)
    table[2 * N_DEV + 64] = 1.0 - 2.0 * (z % 2)
    return split_np(table)


def real_form(frac):
    angle = 2.0 * np.pi * (frac % 1.0)
    cos, sin = np.cos(angle), np.sin(angle)
    return np.block([[cos, sin], [-sin, cos]])


def device_table():
    s = np.arange(N_DEV)
    i, q = s // N_PY, s % N_PY
    return split_np(real_form(np.outer(i, i) / N_PX + np.outer(q, q) / N_PY))


def lane_table():
    m = np.arange(128)
    b, y = m // 8, m % 8
    return split_np(real_form(np.outer(b, b) / 16.0 + np.outer(y, y) / 8.0).T)


def twiddles():
    angle_x = 2.0 * np.pi * np.outer(np.arange(N_PX), LANE_CX) / NG
    angle_y = 2.0 * np.pi * np.outer(np.arange(N_PY), LANE_CY) / NG
    tw_x = np.stack([np.cos(angle_x), np.sin(angle_x)]).astype(np.float32)
    tw_y = np.stack([np.cos(angle_y), np.sin(angle_y)]).astype(np.float32)
    angle2 = 2.0 * np.pi * (LANE_B * LANE_A / 48.0 + LANE_Y * LANE_A2 / 24.0)
    tw2 = np.zeros((8, ROWS), np.float32)
    tw2[0], tw2[1] = np.cos(angle2), np.sin(angle2)
    return tw_x, tw_y, tw2


def split(value):
    high = value.astype(BF)
    return high, (value - high.astype(F32)).astype(BF)


def dot(left, right, dims=NN):
    return lax.dot_general(left, right, (dims, ((), ())), preferred_element_type=F32)


def dot3(left, right, dims=NN):
    (left_dim,), (right_dim,) = dims
    return dot(
        jnp.concatenate([left[0], left[1], left[0]], axis=left_dim),
        jnp.concatenate([right[0], right[0], right[1]], axis=right_dim),
        dims,
    )


def window_kernel(kz_ref, out):
    step = 64

    def block(index, carry):
        kz = kz_ref[index // (ROWS // step)]
        begin = pl.multiple_of((index % (ROWS // step)) * step, step)
        row = lax.broadcasted_iota(jnp.int32, (step, 128), 0) + begin
        lane = lax.broadcasted_iota(jnp.int32, (step, 128), 1)
        u, k1 = begin // N_DEV, row & (N_DEV - 1)
        kx = (k1 >> 4) + N_PX * (u // 3 + 3 * (lane >> 3))
        ky = (k1 & 15) + N_PY * (u % 3 + 3 * (lane & 7))
        fx = jnp.where(kx < NG // 2, kx, kx - NG)
        fy = jnp.where(ky < NG // 2, ky, ky - NG)
        square = (fx * fx + fy * fy + kz * kz).astype(F32)
        radial = jnp.sqrt(square) * (2.0 * math.pi * RADIUS / NG)
        safe = jnp.where(radial > 0, radial, 1.0)
        value = 3.0 * (jnp.sin(safe) - safe * jnp.cos(safe)) / (safe * safe * safe)
        value = jnp.where(radial > 0, value, 1.0)
        both = (kz > 0) & (kz < NG // 2)
        scale = jnp.where(both, 2.0 / float(NG) ** 3, 1.0 / float(NG) ** 3)
        out[index // (ROWS // step), pl.ds(begin, step), :] = value * scale
        return carry

    lax.fori_loop(0, 2 * ROWS // step, block, 0)


def sort_kernel(photons, cells, counts, owners, out):
    blocks = photons.shape[0]
    slots = N_PY * CAP
    target = owners[...]
    hot = jnp.where(
        lax.broadcasted_iota(jnp.int32, (N_PY, blocks), 0) == target, 1.0, 0.0
    )
    before = jnp.where(
        lax.broadcasted_iota(jnp.int32, (blocks, blocks), 0)
        < lax.broadcasted_iota(jnp.int32, (blocks, blocks), 1),
        1.0,
        0.0,
    )
    rank = jnp.sum(dot(hot.astype(BF), before.astype(BF)) * hot, axis=0, keepdims=True)
    place = target * CAP + rank.astype(jnp.int32)
    place_hot = jnp.where(
        lax.broadcasted_iota(jnp.int32, (slots, blocks), 0) == place, 1.0, 0.0
    )
    count = jnp.sum(place_hot * counts[...].astype(F32), axis=1, keepdims=True)
    live = lax.broadcasted_iota(jnp.int32, (slots, SLOTS), 1) < count.astype(jnp.int32)
    place_hot = place_hot.astype(BF)
    for half, value in enumerate((photons[...], cells[...].astype(F32))):
        rest, total = value, None
        for _ in range(3):
            first = rest.astype(BF)
            rest = rest - first.astype(F32)
            part = dot(place_hot, first)
            total = part if total is None else total + part
        out[pl.ds(half, slots, stride=2), :] = jnp.where(live, total, 0.0)


def z_density_kernel(density, t_high, t_low, out, few, high, low):
    for a in range(3):
        for a2 in range(3):
            block = density[a * 16 : (a + 1) * 16, a2 * 8 : (a2 + 1) * 8, :].reshape(128, NG)
            at = slice((a * 3 + a2) * 128, (a * 3 + a2 + 1) * 128)
            high[at, :], low[at, :] = split(block)
    for a in range(3):
        at = slice(a * NG, (a + 1) * NG)
        value = dot3((t_high[...], t_low[...]), (high[at, :], low[at, :]), NT)
        for c in range(2):
            store_plane(out, c * LB + 3 * a, WIDTH, value[c * N_DEV : (c + 1) * N_DEV])
        few[:, at] = value[2 * N_DEV :]


def store_plane(out, start, pitch, value):
    for j in range(value.shape[1] // 128):
        rows = pl.ds(start + j, value.shape[0], stride=pitch)
        out[rows, :] = value[:, j * 128 : (j + 1) * 128]


def paint_kernel(weights, cells, counts, z_density, t_high, t_low, out, *scratch):
    fields, high, low = scratch[:FIELDS], scratch[FIELDS], scratch[FIELDS + 1]
    for field in fields:
        field[...] = jnp.zeros(field.shape, F32)
    lane = lax.broadcasted_iota(jnp.int32, (1, 128), 1)

    def block(index, carry):
        count = counts[index]

        def some(begin, step):
            for k in range(begin, begin + step):
                cell = cells[index, k]
                value = weights[index, k]
                row = lax.shift_right_logical(cell, 7)
                here = lane == (jnp.full((1, 128), cell, jnp.int32) & 127)
                fields[k % FIELDS][pl.ds(row, 1), :] += jnp.where(here, value, 0.0)

        def halves(begin, size):
            @pl.when(count > begin)
            def _():
                if size == 16:
                    some(begin, size)
                else:
                    halves(begin, size // 2)
                    halves(begin + size // 2, size // 2)

        halves(0, SLOTS)
        return carry

    lax.fori_loop(0, counts.shape[0], block, 0)
    for part in range(3):
        for a in range(3):
            for a2 in range(3):
                tiles = []
                for b in range(16):
                    row = (16 * a + b) * CY + 8 * a2
                    tile = fields[0][pl.ds(row * 3 + part, 8, stride=3), :]
                    for field in fields[1:]:
                        tile = tile + field[pl.ds(row * 3 + part, 8, stride=3), :]
                    tiles.append(tile)
                at = slice((a * 3 + a2) * 128, (a * 3 + a2 + 1) * 128)
                to = slice(part * 128, (part + 1) * 128)
                high[at, to], low[at, to] = split(jnp.concatenate(tiles, axis=0))
    pitch = 2 * WIDTH
    half = N_DEV // 2
    first = lax.broadcasted_iota(jnp.int32, (half, NG), 0) == 0
    for a in range(3):
        at = slice(a * NG, (a + 1) * NG)
        value = dot3((t_high[...], t_low[...]), (high[at, :], low[at, :]), NT)
        for c in range(2):
            plane = value[c * N_DEV : (c + 1) * N_DEV]
            store_plane(out, WIDTH + c * LB + 3 * a, pitch, plane)
        dens_cos, dens_sin = z_density[:half, at], z_density[half:, at]
        phot_cos, phot_sin = value[2 * N_DEV : 2 * N_DEV + half], value[2 * N_DEV + half :]
        low_rows, top_rows = 3 * a, half * pitch + 3 * a
        store_plane(out, low_rows, pitch, jnp.where(first, phot_cos, dens_cos))
        store_plane(out, low_rows + LB, pitch, jnp.where(first, dens_cos, dens_sin))
        store_plane(out, top_rows, pitch, jnp.where(first, phot_sin, phot_cos))
        store_plane(out, top_rows + LB, pitch, jnp.where(first, dens_sin, phot_sin))


def three(re, im, sign):
    t_re, t_im = re[1] + re[2], im[1] + im[2]
    d_re = (re[1] - re[2]) * (sign * HALF_ROOT3)
    d_im = (im[1] - im[2]) * (sign * HALF_ROOT3)
    m_re, m_im = re[0] - 0.5 * t_re, im[0] - 0.5 * t_im
    return (re[0] + t_re, m_re - d_im, m_re + d_im), (im[0] + t_im, m_im + d_re, m_im - d_re)


def nine(re, im, sign):
    for group in [(0, 1, 2), (3, 4, 5), (6, 7, 8), (0, 3, 6), (1, 4, 7), (2, 5, 8)]:
        new_re, new_im = three([re[g] for g in group], [im[g] for g in group], sign)
        for k, g in enumerate(group):
            re[g], im[g] = new_re[k], new_im[k]


def middle_kernel(planes, got, *rest):
    count = len(TABLE_SHAPES) + (2 if planes == 2 else 1)
    sources, out, rest = rest[:count], rest[count], rest[count + 1 :]
    tables, (tw1, work, r_high, r_low, l_high, l_low, back, sems) = rest[:count], rest[count:]
    dev_high, dev_low, lane_high, lane_low, tw_x, tw_y, tw2, win = tables[:8]
    copies = [
        pltpu.make_async_copy(source, table, sems.at[k])
        for k, (source, table) in enumerate(zip(sources, tables))
    ]
    for copy in copies:
        copy.start()
    first_plane, out_pitch = (1, PITCH) if planes == 2 else (0, WIDTH)
    pitch = planes * WIDTH
    for p in range(planes):
        for c in range(2):
            for j in range(LB):
                high, low = split(got[pl.ds((p * 2 + c) * LB + j, N_DEV, stride=pitch), :])
                at, to = slice(c * N_DEV, (c + 1) * N_DEV), slice(j * 128, (j + 1) * 128)
                r_high[p, at, to] = high
                r_low[p, at, to] = low
    for copy in copies[:7]:
        copy.wait()
    for k in range(N_PX):
        cos_x, sin_x = tw_x[0, k : k + 1, :], tw_x[1, k : k + 1, :]
        cos_y, sin_y = tw_y[0], tw_y[1]
        at = slice(k * N_PY, (k + 1) * N_PY)
        tw1[0, at, :] = cos_x * cos_y - sin_x * sin_y
        tw1[1, at, :] = sin_x * cos_y + cos_x * sin_y
    dev = (dev_high[...], dev_low[...])
    mat = (lane_high[...], lane_low[...])

    def across(p, a):
        at = slice(a * NG, (a + 1) * NG)
        work[p, :, at] = dot3(dev, (r_high[p, :, at], r_low[p, :, at]))

    def row_block(block, offset=0):
        if isinstance(block, int):
            return slice(block * 16 + offset, block * 16 + offset + 16)
        return pl.ds(pl.multiple_of(block * 16 + offset, 16), 16)

    def forward(p, block):
        rows, rows_im = row_block(block), row_block(block, N_DEV)
        re, im = [], []
        for j in range(LB):
            at = slice(j * 128, (j + 1) * 128)
            cos, sin = tw1[0, rows, at], tw1[1, rows, at]
            x, y = work[p, rows, at], work[p, rows_im, at]
            re.append(x * cos + y * sin)
            im.append(y * cos - x * sin)
        nine(re, im, -1.0)
        for j in range(LB):
            at = slice(j * 128, (j + 1) * 128)
            cos, sin = tw2[0:1, at], tw2[1:2, at]
            to = row_block(block, j * N_DEV)
            l_high[p, to, :128], l_low[p, to, :128] = split(re[j] * cos + im[j] * sin)
            l_high[p, to, 128:], l_low[p, to, 128:] = split(im[j] * cos - re[j] * sin)

    def along(p, k):
        at = slice(k * NG, (k + 1) * NG)
        value = dot3((l_high[p, at, :], l_low[p, at, :]), mat)
        w = win[planes - 1 - p, at, :]
        l_high[p, at, :128], l_low[p, at, :128] = split(value[:, :128] * w)
        l_high[p, at, 128:], l_low[p, at, 128:] = split(value[:, 128:] * w)
        back[p, at, :] = dot3((l_high[p, at, :], l_low[p, at, :]), mat, NT)

    def backward(p, block):
        rows, rows_im = row_block(block), row_block(block, N_DEV)
        re, im = [], []
        for j in range(LB):
            at = slice(j * 128, (j + 1) * 128)
            cos, sin = tw2[0:1, at], tw2[1:2, at]
            of = row_block(block, j * N_DEV)
            x, y = back[p, of, :128], back[p, of, 128:]
            re.append(x * cos - y * sin)
            im.append(y * cos + x * sin)
        nine(re, im, 1.0)
        for j in range(LB):
            at = slice(j * 128, (j + 1) * 128)
            cos, sin = tw1[0, rows, at], tw1[1, rows, at]
            r_high[p, rows, at], r_low[p, rows, at] = split(re[j] * cos - im[j] * sin)
            r_high[p, rows_im, at], r_low[p, rows_im, at] = split(im[j] * cos + re[j] * sin)

    def home(p, a):
        at = slice(a * NG, (a + 1) * NG)
        value = dot3(dev, (r_high[p, :, at], r_low[p, :, at]), TN)
        for c in range(2):
            start = (first_plane + p) * WIDTH + c * LB + a * 3
            store_plane(out, start, out_pitch, value[c * N_DEV : (c + 1) * N_DEV])

    def wait_rest():
        for copy in copies[7:]:
            copy.wait()

    stages = [(across, 3), (forward, N_PX), (along, 3), (backward, N_PX), (home, 3)]
    if planes == 1:
        for stage, (work_of, parts) in enumerate(stages):
            if stage == 2:
                wait_rest()
            if parts == N_PX:

                def step(block, carry, work_of=work_of):
                    work_of(0, block)
                    return carry

                lax.fori_loop(0, parts, step, 0)
            else:
                for part in range(parts):
                    work_of(0, part)
        return
    for stage in range(len(stages) + 1):
        if stage == 2:
            wait_rest()
        both = []
        for p in range(2):
            if 0 <= stage - p < len(stages):
                work_of, parts = stages[stage - p]
                both += [((k + 0.5) / parts, p, work_of, k) for k in range(parts)]
        for _, p, work_of, part in sorted(both, key=lambda item: item[:2]):
            work_of(p, part)
    for j in range(WIDTH):
        out[pl.ds(j, N_DEV, stride=PITCH), :] = tables[8][pl.ds(j, N_DEV, stride=WIDTH), :]


def z_last_kernel(got, t_high, t_low, out):
    a = pl.program_id(0)
    half = N_DEV // 2
    first = lax.broadcasted_iota(jnp.int32, (half, 128), 0) == 0
    dens, phot = [], []
    for a2 in range(3):

        def load(plane, c, begin=0, count=N_DEV):
            start = begin * PITCH + (plane * 2 + c) * LB + a * 3 + a2
            return got[pl.ds(start, count, stride=PITCH), :]

        re_low, im_low = load(1, 0, 0, half), load(1, 1, 0, half)
        re_top, im_top = load(1, 0, half, half), load(1, 1, half, half)
        dens.append(
            jnp.concatenate(
                [
                    load(0, 0),
                    load(0, 1),
                    jnp.where(first, im_low, re_low),
                    jnp.where(first, im_top, im_low),
                ],
                axis=0,
            )
        )
        phot.append(
            jnp.concatenate(
                [
                    load(2, 0),
                    load(2, 1),
                    jnp.where(first, re_low, re_top),
                    jnp.where(first, re_top, im_top),
                ],
                axis=0,
            )
        )
    table = (t_high[...], t_low[...])
    smooth_d = dot3(split(jnp.concatenate(dens, axis=1)), table, TN)
    smooth_p = dot3(split(jnp.concatenate(phot, axis=1)), table, TN)
    value = jnp.clip(smooth_p / jnp.maximum(smooth_d, 0.5), 0.0, 1.0)
    for a2 in range(3):
        out[:, a2 * 8 : (a2 + 1) * 8, :] = value[a2 * 128 : (a2 + 1) * 128].reshape(16, 8, NG)


TABLE_SHAPES = [((256, 256), BF)] * 4 + [
    ((2, N_PX, ROWS), F32),
    ((2, N_PY, ROWS), F32),
    ((8, ROWS), F32),
]


def placed_in(space, *arrays):
    return [pltpu.with_memory_space_constraint(jnp.asarray(a), space) for a in arrays]


def limit(mib):
    return pltpu.CompilerParams(vmem_limit_bytes=mib * 2**20)


def exchange(rows):
    send = rows.reshape(N_DEV, 1, rows.size // N_DEV)
    return lax.all_to_all(send, AXES, 0, 0, tiled=True).reshape(rows.shape)


def middle(got, planes, sources):
    shapes = TABLE_SHAPES + [(source.shape, F32) for source in sources[len(TABLE_SHAPES) :]]
    if planes == 2:
        out_shape = pltpu.VMEM((N_DEV * PITCH, 128), F32)
    else:
        out_shape = jax.ShapeDtypeStruct((N_DEV * WIDTH, 128), F32)
    return pl.pallas_call(
        functools.partial(middle_kernel, planes),
        out_shape=out_shape,
        in_specs=[pl.BlockSpec(memory_space=pltpu.VMEM)]
        + [pl.BlockSpec(memory_space=pl.ANY)] * len(shapes),
        scratch_shapes=[pltpu.VMEM(*shape) for shape in shapes]
        + [
            pltpu.VMEM((2, N_DEV, ROWS), F32),
            pltpu.VMEM((planes, 2 * N_DEV, ROWS), F32),
            pltpu.VMEM((planes, 2 * N_DEV, ROWS), BF),
            pltpu.VMEM((planes, 2 * N_DEV, ROWS), BF),
            pltpu.VMEM((planes, ROWS, 256), BF),
            pltpu.VMEM((planes, ROWS, 256), BF),
            pltpu.VMEM((planes, ROWS, 256), F32),
            pltpu.SemaphoreType.DMA((len(shapes),)),
        ],
        compiler_params=limit(24),
        name=f"middle{planes}",
    )(*placed_in(pltpu.VMEM, got), *placed_in(pltpu.HBM, *sources))


def on_device(photons, halo_cells, halo_counts, owners, density):
    table = z_table()
    tables = (*device_table(), *lane_table(), *twiddles())

    send = pl.pallas_call(
        sort_kernel,
        out_shape=jax.ShapeDtypeStruct((N_PY * CAP * 2, SLOTS), F32),
        name="sort",
    )(photons, halo_cells, halo_counts.reshape(1, -1), owners.reshape(1, -1))
    halos = lax.all_to_all(send.reshape(N_PY, 2 * CAP, SLOTS), "py", 0, 0, tiled=True)

    send_a, few = pl.pallas_call(
        z_density_kernel,
        out_shape=(
            jax.ShapeDtypeStruct((N_DEV * WIDTH, 128), F32),
            jax.ShapeDtypeStruct((N_DEV, ROWS), F32),
        ),
        scratch_shapes=[pltpu.VMEM((ROWS, NG), BF), pltpu.VMEM((ROWS, NG), BF)],
        name="zdensity",
    )(density, *table)
    send_a, halos = lax.optimization_barrier((send_a, halos))
    got_a = exchange(send_a)

    halos = halos.reshape(N_PY * CAP, 2, SLOTS)
    weights, cells = halos[:, 0], halos[:, 1].astype(jnp.int32)
    slot = jnp.arange(1, SLOTS + 1, dtype=jnp.int32)[None, :]
    counts = jnp.max(jnp.where(weights != 0, slot, 0), axis=1)
    smem = pl.BlockSpec(memory_space=pltpu.SMEM)
    vmem = pl.BlockSpec(memory_space=pltpu.VMEM)
    send_bc = pl.pallas_call(
        paint_kernel,
        out_shape=jax.ShapeDtypeStruct((N_DEV * 2 * WIDTH, 128), F32),
        in_specs=[smem, smem, smem, vmem, vmem, vmem],
        scratch_shapes=[pltpu.VMEM((ROWS * 3, 128), F32)] * FIELDS
        + [pltpu.VMEM((ROWS, NG), BF), pltpu.VMEM((ROWS, NG), BF)],
        name="paint",
    )(weights, cells, counts, few, *table)
    got_bc = exchange(send_bc)

    me = lax.axis_index(AXES)
    half = N_DEV // 2
    low = jnp.where(me % half == 0, (me // half) * (NG // 2), me % half)
    win = pl.pallas_call(
        window_kernel,
        out_shape=jax.ShapeDtypeStruct((2, ROWS, 128), F32),
        in_specs=[smem],
        name="window",
    )(jnp.stack([me + 64, low]).astype(jnp.int32))
    back_a = middle(got_a, 1, (*tables, win))
    back = middle(got_bc, 2, (*tables, win, back_a))
    got = exchange(back)
    whole = pl.BlockSpec((N_DEV * PITCH, 128), lambda i: (0, 0))
    whole_t = pl.BlockSpec((3 * N_DEV, NG), lambda i: (0, 0))
    return pl.pallas_call(
        z_last_kernel,
        grid=(3,),
        in_specs=[whole, whole_t, whole_t],
        out_specs=pl.BlockSpec((16, CY, NG), lambda i: (i, 0, 0)),
        out_shape=jax.ShapeDtypeStruct((CX, CY, NG), F32),
        compiler_params=limit(16),
        name="zlast",
    )(*placed_in(pltpu.VMEM, got, *table))


def solution(mesh):
    placed = (
        P(("px", "py"), None),
        P(("px", "py"), None),
        P(("px", "py")),
        P(("px", "py"), None),
        P("px", "py", None),
    )
    return jax.shard_map(
        on_device, mesh=mesh, in_specs=placed, out_specs=P("px", "py", None), check_vma=False
    )
```

```python
import functools
import math

import jax
import jax.numpy as jnp
import ml_dtypes
import numpy as np
from jax import lax
from jax.experimental import pallas as pl
from jax.experimental.pallas import tpu as pltpu
from jax.sharding import PartitionSpec as P

NG = 384
SLOTS = 128
CAP = 4
RADIUS = 20
N_PX = 8
N_PY = 16
N_DEV = 128
CX = 48
CY = 24
ROWS = CX * CY
LB = ROWS // 128
PLANES = 3
WIDTH = 2 * LB
PITCH = PLANES * WIDTH
FIELDS = 4
AXES = ("px", "py")
BF = jnp.bfloat16
F32 = jnp.float32
NT = ((1,), (1,))
NN = ((1,), (0,))
TN = ((0,), (0,))
HALF_ROOT3 = math.sqrt(3.0) / 2.0

LANE_A, LANE_A2, LANE_B, LANE_Y = (
    g.reshape(-1) for g in np.meshgrid(range(3), range(3), range(16), range(8), indexing="ij")
)
LANE_CX = 16 * LANE_A + LANE_B
LANE_CY = 8 * LANE_A2 + LANE_Y


def split_np(table):
    high = table.astype(ml_dtypes.bfloat16)
    low = (table - high.astype(np.float64)).astype(ml_dtypes.bfloat16)
    return high, low


def z_tables():
    z = np.arange(128)
    kz = 3 * np.arange(N_DEV // 2)
    angle = 2.0 * np.pi * (np.outer(kz, z) % NG) / NG
    few = np.concatenate([np.cos(angle), np.sin(angle)])
    few[N_DEV // 2] = 1.0 - 2.0 * (z % 2)
    kz = 3 * np.arange(N_DEV) // 2 + 1
    angle = 2.0 * np.pi * (np.outer(kz, z) % NG) / NG
    sign = np.where(kz % 3 == 1, 1.0, -1.0)[:, None]
    cos, sin = np.cos(angle), np.sin(angle)
    many = np.block([[cos, -sign * sin], [sin, sign * cos]])
    return (*split_np(few), *split_np(many))


def real_form(frac):
    angle = 2.0 * np.pi * (frac % 1.0)
    cos, sin = np.cos(angle), np.sin(angle)
    return np.block([[cos, sin], [-sin, cos]])


def device_table():
    s = np.arange(N_DEV)
    i, q = s // N_PY, s % N_PY
    return split_np(real_form(np.outer(i, i) / N_PX + np.outer(q, q) / N_PY))


def lane_table():
    m = np.arange(128)
    b, y = m // 8, m % 8
    return split_np(real_form(np.outer(b, b) / 16.0 + np.outer(y, y) / 8.0).T)


def twiddles():
    angle_x = 2.0 * np.pi * np.outer(np.arange(N_PX), LANE_CX) / NG
    angle_y = 2.0 * np.pi * np.outer(np.arange(N_PY), LANE_CY) / NG
    tw_x = np.stack([np.cos(angle_x), np.sin(angle_x)]).astype(np.float32)
    tw_y = np.stack([np.cos(angle_y), np.sin(angle_y)]).astype(np.float32)
    angle2 = 2.0 * np.pi * (LANE_B * LANE_A / 48.0 + LANE_Y * LANE_A2 / 24.0)
    tw2 = np.zeros((8, ROWS), np.float32)
    tw2[0], tw2[1] = np.cos(angle2), np.sin(angle2)
    return tw_x, tw_y, tw2


def split(value):
    high = value.astype(BF)
    return high, (value - high.astype(F32)).astype(BF)


def dot(left, right, dims=NN):
    return lax.dot_general(left, right, (dims, ((), ())), preferred_element_type=F32)


def dot3(left, right, dims=NN):
    (left_dim,), (right_dim,) = dims
    return dot(
        jnp.concatenate([left[0], left[1], left[0]], axis=left_dim),
        jnp.concatenate([right[0], right[0], right[1]], axis=right_dim),
        dims,
    )


def window_kernel(kz_ref, out):
    step = 64

    def block(index, carry):
        kz = kz_ref[index // (ROWS // step)]
        begin = pl.multiple_of((index % (ROWS // step)) * step, step)
        row = lax.broadcasted_iota(jnp.int32, (step, 128), 0) + begin
        lane = lax.broadcasted_iota(jnp.int32, (step, 128), 1)
        u, k1 = begin // N_DEV, row & (N_DEV - 1)
        kx = (k1 >> 4) + N_PX * (u // 3 + 3 * (lane >> 3))
        ky = (k1 & 15) + N_PY * (u % 3 + 3 * (lane & 7))
        fx = jnp.where(kx < NG // 2, kx, kx - NG)
        fy = jnp.where(ky < NG // 2, ky, ky - NG)
        square = (fx * fx + fy * fy + kz * kz).astype(F32)
        radial = jnp.sqrt(square) * (2.0 * math.pi * RADIUS / NG)
        safe = jnp.where(radial > 0, radial, 1.0)
        value = 3.0 * (jnp.sin(safe) - safe * jnp.cos(safe)) / (safe * safe * safe)
        value = jnp.where(radial > 0, value, 1.0)
        both = (kz > 0) & (kz < NG // 2)
        scale = jnp.where(both, 2.0 / float(NG) ** 3, 1.0 / float(NG) ** 3)
        out[index // (ROWS // step), pl.ds(begin, step), :] = value * scale
        return carry

    lax.fori_loop(0, 2 * ROWS // step, block, 0)


def sort_kernel(photons, cells, counts, owners, out):
    blocks = photons.shape[0]
    slots = N_PY * CAP
    target = owners[...]
    hot = jnp.where(
        lax.broadcasted_iota(jnp.int32, (N_PY, blocks), 0) == target, 1.0, 0.0
    )
    before = jnp.where(
        lax.broadcasted_iota(jnp.int32, (blocks, blocks), 0)
        < lax.broadcasted_iota(jnp.int32, (blocks, blocks), 1),
        1.0,
        0.0,
    )
    rank = jnp.sum(dot(hot.astype(BF), before.astype(BF)) * hot, axis=0, keepdims=True)
    place = target * CAP + rank.astype(jnp.int32)
    place_hot = jnp.where(
        lax.broadcasted_iota(jnp.int32, (slots, blocks), 0) == place, 1.0, 0.0
    )
    count = jnp.sum(place_hot * counts[...].astype(F32), axis=1, keepdims=True)
    live = lax.broadcasted_iota(jnp.int32, (slots, SLOTS), 1) < count.astype(jnp.int32)
    place_hot = place_hot.astype(BF)
    for half, value in enumerate((photons[...], cells[...].astype(F32))):
        rest, total = value, None
        for _ in range(3):
            first = rest.astype(BF)
            rest = rest - first.astype(F32)
            part = dot(place_hot, first)
            total = part if total is None else total + part
        out[pl.ds(half, slots, stride=2), :] = jnp.where(live, total, 0.0)


def fold(parts):
    t = parts[1] + parts[2]
    return parts[0] + t, parts[0] - 0.5 * t, (parts[1] - parts[2]) * HALF_ROOT3


def z_density_kernel(density, few_high, few_low, many_high, many_low, out, few, *scratch):
    high0, low0, high1, low1 = scratch
    for a in range(3):
        for a2 in range(3):
            at = slice((a * 3 + a2) * 128, (a * 3 + a2 + 1) * 128)
            block = density[a * 16 : (a + 1) * 16, a2 * 8 : (a2 + 1) * 8, :].reshape(128, NG)
            store_folded(scratch, at, fold([block[:, k * 128 : (k + 1) * 128] for k in range(3)]))
    for a in range(3):
        at = slice(a * NG, (a + 1) * NG)
        value = dot3((many_high[...], many_low[...]), (high1[at, :], low1[at, :]), NT)
        for c in range(2):
            store_plane(out, c * LB + 3 * a, WIDTH, value[c * N_DEV : (c + 1) * N_DEV])
        few[:, at] = dot3((few_high[...], few_low[...]), (high0[at, :], low0[at, :]), NT)


def store_folded(scratch, at, folded):
    high0, low0, high1, low1 = scratch
    high0[at, :], low0[at, :] = split(folded[0])
    high1[at, :128], low1[at, :128] = split(folded[1])
    high1[at, 128:], low1[at, 128:] = split(folded[2])


def store_plane(out, start, pitch, value):
    for j in range(value.shape[1] // 128):
        rows = pl.ds(start + j, value.shape[0], stride=pitch)
        out[rows, :] = value[:, j * 128 : (j + 1) * 128]


def paint_kernel(weights, cells, counts, z_density, few_high, few_low, many_high, many_low, out,
                 *scratch):
    fields, folded = scratch[:FIELDS], scratch[FIELDS:]
    high0, low0, high1, low1 = folded
    for field in fields:
        field[...] = jnp.zeros(field.shape, F32)
    lane = lax.broadcasted_iota(jnp.int32, (1, 128), 1)

    def block(index, carry):
        count = counts[index]

        def some(begin, step):
            for k in range(begin, begin + step):
                cell = cells[index, k]
                value = weights[index, k]
                row = lax.shift_right_logical(cell, 7)
                here = lane == (jnp.full((1, 128), cell, jnp.int32) & 127)
                fields[k % FIELDS][pl.ds(row, 1), :] += jnp.where(here, value, 0.0)

        def halves(begin, size):
            @pl.when(count > begin)
            def _():
                if size == 16:
                    some(begin, size)
                else:
                    halves(begin, size // 2)
                    halves(begin + size // 2, size // 2)

        halves(0, SLOTS)
        return carry

    lax.fori_loop(0, counts.shape[0], block, 0)
    for a in range(3):
        for a2 in range(3):
            parts = []
            for part in range(3):
                tiles = []
                for b in range(16):
                    row = (16 * a + b) * CY + 8 * a2
                    tile = fields[0][pl.ds(row * 3 + part, 8, stride=3), :]
                    for field in fields[1:]:
                        tile = tile + field[pl.ds(row * 3 + part, 8, stride=3), :]
                    tiles.append(tile)
                parts.append(jnp.concatenate(tiles, axis=0))
            at = slice((a * 3 + a2) * 128, (a * 3 + a2 + 1) * 128)
            store_folded(folded, at, fold(parts))
    pitch = 2 * WIDTH
    half = N_DEV // 2
    first = lax.broadcasted_iota(jnp.int32, (half, NG), 0) == 0
    for a in range(3):
        at = slice(a * NG, (a + 1) * NG)
        value = dot3((many_high[...], many_low[...]), (high1[at, :], low1[at, :]), NT)
        for c in range(2):
            plane = value[c * N_DEV : (c + 1) * N_DEV]
            store_plane(out, WIDTH + c * LB + 3 * a, pitch, plane)
        dens_cos, dens_sin = z_density[:half, at], z_density[half:, at]
        value = dot3((few_high[...], few_low[...]), (high0[at, :], low0[at, :]), NT)
        phot_cos, phot_sin = value[:half], value[half:]
        low_rows, top_rows = 3 * a, half * pitch + 3 * a
        store_plane(out, low_rows, pitch, jnp.where(first, phot_cos, dens_cos))
        store_plane(out, low_rows + LB, pitch, jnp.where(first, dens_cos, dens_sin))
        store_plane(out, top_rows, pitch, jnp.where(first, phot_sin, phot_cos))
        store_plane(out, top_rows + LB, pitch, jnp.where(first, dens_sin, phot_sin))


def three(re, im, sign):
    t_re, t_im = re[1] + re[2], im[1] + im[2]
    d_re = (re[1] - re[2]) * (sign * HALF_ROOT3)
    d_im = (im[1] - im[2]) * (sign * HALF_ROOT3)
    m_re, m_im = re[0] - 0.5 * t_re, im[0] - 0.5 * t_im
    return (re[0] + t_re, m_re - d_im, m_re + d_im), (im[0] + t_im, m_im + d_re, m_im - d_re)


def nine(re, im, sign):
    for group in [(0, 1, 2), (3, 4, 5), (6, 7, 8), (0, 3, 6), (1, 4, 7), (2, 5, 8)]:
        new_re, new_im = three([re[g] for g in group], [im[g] for g in group], sign)
        for k, g in enumerate(group):
            re[g], im[g] = new_re[k], new_im[k]


def middle_kernel(planes, got, *rest):
    count = len(TABLE_SHAPES) + (2 if planes == 2 else 1)
    sources, out, rest = rest[:count], rest[count], rest[count + 1 :]
    tables, (tw1, work, r_high, r_low, l_high, l_low, back, sems) = rest[:count], rest[count:]
    dev_high, dev_low, tw_x, tw_y, tw2, lane_high, lane_low, win = tables[:8]
    copies = [
        pltpu.make_async_copy(source, table, sems.at[k])
        for k, (source, table) in enumerate(zip(sources, tables))
    ]
    for copy in copies:
        copy.start()
    first_plane, out_pitch = (1, PITCH) if planes == 2 else (0, WIDTH)
    pitch = planes * WIDTH
    for p in range(planes):
        for c in range(2):
            for j in range(LB):
                high, low = split(got[pl.ds((p * 2 + c) * LB + j, N_DEV, stride=pitch), :])
                at, to = slice(c * N_DEV, (c + 1) * N_DEV), slice(j * 128, (j + 1) * 128)
                r_high[p, at, to] = high
                r_low[p, at, to] = low

    def dev():
        return dev_high[...], dev_low[...]

    def mat():
        return lane_high[...], lane_low[...]

    def arrive(stage):
        if stage < 3:
            for copy in copies[(0, 2, 5)[stage] : (2, 5, len(copies))[stage]]:
                copy.wait()
        if stage == 1:
            for k in range(N_PX):
                cos_x, sin_x = tw_x[0, k : k + 1, :], tw_x[1, k : k + 1, :]
                cos_y, sin_y = tw_y[0], tw_y[1]
                at = slice(k * N_PY, (k + 1) * N_PY)
                tw1[0, at, :] = cos_x * cos_y - sin_x * sin_y
                tw1[1, at, :] = sin_x * cos_y + cos_x * sin_y

    def across(p, a):
        at = slice(a * NG, (a + 1) * NG)
        work[p, :, at] = dot3(dev(), (r_high[p, :, at], r_low[p, :, at]))

    def row_block(block, offset=0):
        if isinstance(block, int):
            return slice(block * 16 + offset, block * 16 + offset + 16)
        return pl.ds(pl.multiple_of(block * 16 + offset, 16), 16)

    def forward(p, block):
        rows, rows_im = row_block(block), row_block(block, N_DEV)
        re, im = [], []
        for j in range(LB):
            at = slice(j * 128, (j + 1) * 128)
            cos, sin = tw1[0, rows, at], tw1[1, rows, at]
            x, y = work[p, rows, at], work[p, rows_im, at]
            re.append(x * cos + y * sin)
            im.append(y * cos - x * sin)
        nine(re, im, -1.0)
        for j in range(LB):
            at = slice(j * 128, (j + 1) * 128)
            cos, sin = tw2[0:1, at], tw2[1:2, at]
            to = row_block(block, j * N_DEV)
            l_high[p, to, :128], l_low[p, to, :128] = split(re[j] * cos + im[j] * sin)
            l_high[p, to, 128:], l_low[p, to, 128:] = split(im[j] * cos - re[j] * sin)

    def along(p, k):
        at = slice(k * NG, (k + 1) * NG)
        value = dot3((l_high[p, at, :], l_low[p, at, :]), mat())
        w = win[planes - 1 - p, at, :]
        l_high[p, at, :128], l_low[p, at, :128] = split(value[:, :128] * w)
        l_high[p, at, 128:], l_low[p, at, 128:] = split(value[:, 128:] * w)
        back[p, at, :] = dot3((l_high[p, at, :], l_low[p, at, :]), mat(), NT)

    def backward(p, block):
        rows, rows_im = row_block(block), row_block(block, N_DEV)
        re, im = [], []
        for j in range(LB):
            at = slice(j * 128, (j + 1) * 128)
            cos, sin = tw2[0:1, at], tw2[1:2, at]
            of = row_block(block, j * N_DEV)
            x, y = back[p, of, :128], back[p, of, 128:]
            re.append(x * cos - y * sin)
            im.append(y * cos + x * sin)
        nine(re, im, 1.0)
        for j in range(LB):
            at = slice(j * 128, (j + 1) * 128)
            cos, sin = tw1[0, rows, at], tw1[1, rows, at]
            r_high[p, rows, at], r_low[p, rows, at] = split(re[j] * cos - im[j] * sin)
            r_high[p, rows_im, at], r_low[p, rows_im, at] = split(im[j] * cos + re[j] * sin)

    def home(p, a):
        at = slice(a * NG, (a + 1) * NG)
        value = dot3(dev(), (r_high[p, :, at], r_low[p, :, at]), TN)
        for c in range(2):
            start = (first_plane + p) * WIDTH + c * LB + a * 3
            store_plane(out, start, out_pitch, value[c * N_DEV : (c + 1) * N_DEV])

    stages = [(across, 3), (forward, N_PX), (along, 3), (backward, N_PX), (home, 3)]
    if planes == 1:
        for stage, (work_of, parts) in enumerate(stages):
            arrive(stage)
            if parts == N_PX:

                def step(block, carry, work_of=work_of):
                    work_of(0, block)
                    return carry

                lax.fori_loop(0, parts, step, 0)
            else:
                for part in range(parts):
                    work_of(0, part)
        return
    for stage in range(len(stages) + 1):
        arrive(stage)
        both = []
        for p in range(2):
            if 0 <= stage - p < len(stages):
                work_of, parts = stages[stage - p]
                both += [((k + 0.5) / parts, p, work_of, k) for k in range(parts)]
        for _, p, work_of, part in sorted(both, key=lambda item: item[:2]):
            work_of(p, part)
    for j in range(WIDTH):
        out[pl.ds(j, N_DEV, stride=PITCH), :] = tables[8][pl.ds(j, N_DEV, stride=WIDTH), :]


def z_last_kernel(got, few_high, few_low, many_high, many_low, out):
    a = pl.program_id(0)
    half = N_DEV // 2
    first = lax.broadcasted_iota(jnp.int32, (half, 128), 0) == 0
    many, few = [[], []], [[], []]
    for a2 in range(3):

        def load(plane, c, begin=0, count=N_DEV):
            start = begin * PITCH + (plane * 2 + c) * LB + a * 3 + a2
            return got[pl.ds(start, count, stride=PITCH), :]

        re_low, im_low = load(1, 0, 0, half), load(1, 1, 0, half)
        re_top, im_top = load(1, 0, half, half), load(1, 1, half, half)
        many[0].append(jnp.concatenate([load(0, 0), load(0, 1)], axis=0))
        many[1].append(jnp.concatenate([load(2, 0), load(2, 1)], axis=0))
        dens = [jnp.where(first, im_low, re_low), jnp.where(first, im_top, im_low)]
        phot = [jnp.where(first, re_low, re_top), jnp.where(first, re_top, im_top)]
        few[0].append(jnp.concatenate(dens, axis=0))
        few[1].append(jnp.concatenate(phot, axis=0))
    smooth = []
    for k in range(2):
        same = dot3(split(jnp.concatenate(few[k], axis=1)), (few_high[...], few_low[...]), TN)
        turn = dot3(split(jnp.concatenate(many[k], axis=1)), (many_high[...], many_low[...]), TN)
        even, odd = turn[:, :128], turn[:, 128:] * HALF_ROOT3
        rest = same - 0.5 * even
        smooth.append((same + even, rest + odd, rest - odd))
    for k in range(3):
        value = jnp.clip(smooth[1][k] / jnp.maximum(smooth[0][k], 0.5), 0.0, 1.0)
        for a2 in range(3):
            block = value[a2 * 128 : (a2 + 1) * 128].reshape(16, 8, 128)
            out[:, a2 * 8 : (a2 + 1) * 8, k * 128 : (k + 1) * 128] = block


SQUARE = [((256, 256), BF)] * 2
TABLE_SHAPES = [
    *SQUARE,
    ((2, N_PX, ROWS), F32),
    ((2, N_PY, ROWS), F32),
    ((8, ROWS), F32),
    *SQUARE,
]
FOLDED = [pltpu.VMEM((ROWS, width), BF) for width in (128, 128, 256, 256)]


def placed_in(space, *arrays):
    return [pltpu.with_memory_space_constraint(jnp.asarray(a), space) for a in arrays]


def limit(mib):
    return pltpu.CompilerParams(vmem_limit_bytes=mib * 2**20)


def exchange(rows):
    send = rows.reshape(N_DEV, 1, rows.size // N_DEV)
    return lax.all_to_all(send, AXES, 0, 0, tiled=True).reshape(rows.shape)


def middle(got, planes, sources):
    shapes = TABLE_SHAPES + [(source.shape, F32) for source in sources[len(TABLE_SHAPES) :]]
    if planes == 2:
        out_shape = pltpu.VMEM((N_DEV * PITCH, 128), F32)
    else:
        out_shape = jax.ShapeDtypeStruct((N_DEV * WIDTH, 128), F32)
    return pl.pallas_call(
        functools.partial(middle_kernel, planes),
        out_shape=out_shape,
        in_specs=[pl.BlockSpec(memory_space=pltpu.VMEM)]
        + [pl.BlockSpec(memory_space=pl.ANY)] * len(shapes),
        scratch_shapes=[pltpu.VMEM(*shape) for shape in shapes]
        + [
            pltpu.VMEM((2, N_DEV, ROWS), F32),
            pltpu.VMEM((planes, 2 * N_DEV, ROWS), F32),
            pltpu.VMEM((planes, 2 * N_DEV, ROWS), BF),
            pltpu.VMEM((planes, 2 * N_DEV, ROWS), BF),
            pltpu.VMEM((planes, ROWS, 256), BF),
            pltpu.VMEM((planes, ROWS, 256), BF),
            pltpu.VMEM((planes, ROWS, 256), F32),
            pltpu.SemaphoreType.DMA((len(shapes),)),
        ],
        compiler_params=limit(24),
        name=f"middle{planes}",
    )(*placed_in(pltpu.VMEM, got), *placed_in(pltpu.HBM, *sources))


def on_device(photons, halo_cells, halo_counts, owners, density):
    table = z_tables()
    tables = (*device_table(), *twiddles(), *lane_table())

    send = pl.pallas_call(
        sort_kernel,
        out_shape=jax.ShapeDtypeStruct((N_PY * CAP * 2, SLOTS), F32),
        name="sort",
    )(photons, halo_cells, halo_counts.reshape(1, -1), owners.reshape(1, -1))
    halos = lax.all_to_all(send.reshape(N_PY, 2 * CAP, SLOTS), "py", 0, 0, tiled=True)

    send_a, few = pl.pallas_call(
        z_density_kernel,
        out_shape=(
            jax.ShapeDtypeStruct((N_DEV * WIDTH, 128), F32),
            jax.ShapeDtypeStruct((N_DEV, ROWS), F32),
        ),
        scratch_shapes=FOLDED,
        name="zdensity",
    )(density, *table)
    send_a, halos = lax.optimization_barrier((send_a, halos))
    got_a = exchange(send_a)

    halos = halos.reshape(N_PY * CAP, 2, SLOTS)
    weights, cells = halos[:, 0], halos[:, 1].astype(jnp.int32)
    slot = jnp.arange(1, SLOTS + 1, dtype=jnp.int32)[None, :]
    counts = jnp.max(jnp.where(weights != 0, slot, 0), axis=1)
    smem = pl.BlockSpec(memory_space=pltpu.SMEM)
    vmem = pl.BlockSpec(memory_space=pltpu.VMEM)
    send_bc = pl.pallas_call(
        paint_kernel,
        out_shape=jax.ShapeDtypeStruct((N_DEV * 2 * WIDTH, 128), F32),
        in_specs=[smem, smem, smem] + [vmem] * 5,
        scratch_shapes=[pltpu.VMEM((ROWS * 3, 128), F32)] * FIELDS
        + FOLDED,
        name="paint",
    )(weights, cells, counts, few, *table)
    got_bc = exchange(send_bc)

    me = lax.axis_index(AXES)
    half = N_DEV // 2
    high = 3 * me // 2 + 1
    low = jnp.where(me % half == 0, (me // half) * (NG // 2), 3 * (me % half))
    win = pl.pallas_call(
        window_kernel,
        out_shape=jax.ShapeDtypeStruct((2, ROWS, 128), F32),
        in_specs=[smem],
        name="window",
    )(jnp.stack([high, low]).astype(jnp.int32))
    back_a = middle(got_a, 1, (*tables, win))
    back = middle(got_bc, 2, (*tables, win, back_a))
    got = exchange(back)
    whole = pl.BlockSpec((N_DEV * PITCH, 128), lambda i: (0, 0))
    whole_t = [pl.BlockSpec(t.shape, lambda i: (0, 0)) for t in table]
    return pl.pallas_call(
        z_last_kernel,
        grid=(3,),
        in_specs=[whole] + whole_t,
        out_specs=pl.BlockSpec((16, CY, NG), lambda i: (i, 0, 0)),
        out_shape=jax.ShapeDtypeStruct((CX, CY, NG), F32),
        compiler_params=limit(16),
        name="zlast",
    )(*placed_in(pltpu.VMEM, got, *table))


def solution(mesh):
    placed = (
        P(("px", "py"), None),
        P(("px", "py"), None),
        P(("px", "py")),
        P(("px", "py"), None),
        P("px", "py", None),
    )
    return jax.shard_map(
        on_device, mesh=mesh, in_specs=placed, out_specs=P("px", "py", None), check_vma=False
    )
```

```python
import functools
import math

import jax
import jax.numpy as jnp
import ml_dtypes
import numpy as np
from jax import lax
from jax.experimental import pallas as pl
from jax.experimental.pallas import tpu as pltpu
from jax.sharding import PartitionSpec as P

NG = 384
SLOTS = 128
CAP = 4
RADIUS = 20
N_PX = 8
N_PY = 16
N_DEV = 128
CX = 48
CY = 24
ROWS = CX * CY
LB = ROWS // 128
PLANES = 3
WIDTH = 2 * LB
PITCH = PLANES * WIDTH
FIELDS = 4
AXES = ("px", "py")
BF = jnp.bfloat16
F32 = jnp.float32
NT = ((1,), (1,))
NN = ((1,), (0,))
TN = ((0,), (0,))
HALF_ROOT3 = math.sqrt(3.0) / 2.0

LANE_A, LANE_A2, LANE_B, LANE_Y = (
    g.reshape(-1) for g in np.meshgrid(range(3), range(3), range(16), range(8), indexing="ij")
)
LANE_CX = 16 * LANE_A + LANE_B
LANE_CY = 8 * LANE_A2 + LANE_Y


def split_np(table):
    high = table.astype(ml_dtypes.bfloat16)
    low = (table - high.astype(np.float64)).astype(ml_dtypes.bfloat16)
    return high, low


def z_tables():
    z = np.arange(128)
    kz = 3 * np.arange(N_DEV // 2)
    angle = 2.0 * np.pi * (np.outer(kz, z) % NG) / NG
    few = np.concatenate([np.cos(angle), np.sin(angle)])
    few[N_DEV // 2] = 1.0 - 2.0 * (z % 2)
    kz = 3 * np.arange(N_DEV) // 2 + 1
    angle = 2.0 * np.pi * (np.outer(kz, z) % NG) / NG
    sign = np.where(kz % 3 == 1, 1.0, -1.0)[:, None]
    cos, sin = np.cos(angle), np.sin(angle)
    many = np.block([[cos, -sign * sin], [sin, sign * cos]])
    return (*split_np(few), *split_np(many))


def real_form(frac):
    angle = 2.0 * np.pi * (frac % 1.0)
    cos, sin = np.cos(angle), np.sin(angle)
    return np.block([[cos, sin], [-sin, cos]])


def device_table():
    s = np.arange(N_DEV)
    i, q = s // N_PY, s % N_PY
    form = real_form(np.outer(i, i) / N_PX + np.outer(q, q) / N_PY)
    return split_np(form), split_np(form.T)


def lane_table():
    m = np.arange(128)
    b, y = m // 8, m % 8
    form = real_form(np.outer(b, b) / 16.0 + np.outer(y, y) / 8.0)
    return split_np(form.T), split_np(form)


def twiddles():
    angle_x = 2.0 * np.pi * np.outer(np.arange(N_PX), LANE_CX) / NG
    angle_y = 2.0 * np.pi * np.outer(np.arange(N_PY), LANE_CY) / NG
    tw_x = np.stack([np.cos(angle_x), np.sin(angle_x)]).astype(np.float32)
    tw_y = np.stack([np.cos(angle_y), np.sin(angle_y)]).astype(np.float32)
    angle2 = 2.0 * np.pi * (LANE_B * LANE_A / 48.0 + LANE_Y * LANE_A2 / 24.0)
    tw2 = np.zeros((8, ROWS), np.float32)
    tw2[0], tw2[1] = np.cos(angle2), np.sin(angle2)
    return tw_x, tw_y, tw2


def split(value):
    high = value.astype(BF)
    return high, (value - high.astype(F32)).astype(BF)


def dot(left, right, dims=NN):
    return lax.dot_general(left, right, (dims, ((), ())), preferred_element_type=F32)


def dot3(left, right, dims=NN):
    (left_dim,), (right_dim,) = dims
    return dot(
        jnp.concatenate([left[0], left[1], left[0]], axis=left_dim),
        jnp.concatenate([right[0], right[0], right[1]], axis=right_dim),
        dims,
    )


def window_kernel(kz_ref, out):
    step = 64

    def block(index, carry):
        kz = kz_ref[index // (ROWS // step)]
        begin = pl.multiple_of((index % (ROWS // step)) * step, step)
        row = lax.broadcasted_iota(jnp.int32, (step, 128), 0) + begin
        lane = lax.broadcasted_iota(jnp.int32, (step, 128), 1)
        u, k1 = begin // N_DEV, row & (N_DEV - 1)
        kx = (k1 >> 4) + N_PX * (u // 3 + 3 * (lane >> 3))
        ky = (k1 & 15) + N_PY * (u % 3 + 3 * (lane & 7))
        fx = jnp.where(kx < NG // 2, kx, kx - NG)
        fy = jnp.where(ky < NG // 2, ky, ky - NG)
        square = (fx * fx + fy * fy + kz * kz).astype(F32)
        radial = jnp.sqrt(square) * (2.0 * math.pi * RADIUS / NG)
        safe = jnp.where(radial > 0, radial, 1.0)
        value = 3.0 * (jnp.sin(safe) - safe * jnp.cos(safe)) / (safe * safe * safe)
        value = jnp.where(radial > 0, value, 1.0)
        both = (kz > 0) & (kz < NG // 2)
        scale = jnp.where(both, 2.0 / float(NG) ** 3, 1.0 / float(NG) ** 3)
        out[index // (ROWS // step), pl.ds(begin, step), :] = value * scale
        return carry

    lax.fori_loop(0, 2 * ROWS // step, block, 0)


def sort_kernel(photons, cells, counts, owners, out):
    blocks = photons.shape[0]
    slots = N_PY * CAP
    target = owners[...]
    hot = jnp.where(
        lax.broadcasted_iota(jnp.int32, (N_PY, blocks), 0) == target, 1.0, 0.0
    )
    before = jnp.where(
        lax.broadcasted_iota(jnp.int32, (blocks, blocks), 0)
        < lax.broadcasted_iota(jnp.int32, (blocks, blocks), 1),
        1.0,
        0.0,
    )
    rank = jnp.sum(dot(hot.astype(BF), before.astype(BF)) * hot, axis=0, keepdims=True)
    place = target * CAP + rank.astype(jnp.int32)
    place_hot = jnp.where(
        lax.broadcasted_iota(jnp.int32, (slots, blocks), 0) == place, 1.0, 0.0
    )
    count = jnp.sum(place_hot * counts[...].astype(F32), axis=1, keepdims=True)
    live = lax.broadcasted_iota(jnp.int32, (slots, SLOTS), 1) < count.astype(jnp.int32)
    place_hot = place_hot.astype(BF)
    for half, value in enumerate((photons[...], cells[...].astype(F32))):
        rest, total = value, None
        for _ in range(3):
            first = rest.astype(BF)
            rest = rest - first.astype(F32)
            part = dot(place_hot, first)
            total = part if total is None else total + part
        out[pl.ds(half, slots, stride=2), :] = jnp.where(live, total, 0.0)


def fold(parts):
    t = parts[1] + parts[2]
    return parts[0] + t, parts[0] - 0.5 * t, (parts[1] - parts[2]) * HALF_ROOT3


def z_density_kernel(density, few_high, few_low, many_high, many_low, out, few, *scratch):
    high0, low0, high1, low1 = scratch
    for a in range(3):
        for a2 in range(3):
            at = slice((a * 3 + a2) * 128, (a * 3 + a2 + 1) * 128)
            block = density[a * 16 : (a + 1) * 16, a2 * 8 : (a2 + 1) * 8, :].reshape(128, NG)
            store_folded(scratch, at, fold([block[:, k * 128 : (k + 1) * 128] for k in range(3)]))
    for a in range(3):
        at = slice(a * NG, (a + 1) * NG)
        value = dot3((many_high[...], many_low[...]), (high1[at, :], low1[at, :]), NT)
        for c in range(2):
            store_plane(out, c * LB + 3 * a, WIDTH, value[c * N_DEV : (c + 1) * N_DEV])
        few[:, at] = dot3((few_high[...], few_low[...]), (high0[at, :], low0[at, :]), NT)


def store_folded(scratch, at, folded):
    high0, low0, high1, low1 = scratch
    high0[at, :], low0[at, :] = split(folded[0])
    high1[at, :128], low1[at, :128] = split(folded[1])
    high1[at, 128:], low1[at, 128:] = split(folded[2])


def store_plane(out, start, pitch, value):
    for j in range(value.shape[1] // 128):
        rows = pl.ds(start + j, value.shape[0], stride=pitch)
        out[rows, :] = value[:, j * 128 : (j + 1) * 128]


def paint_kernel(weights, cells, counts, z_density, few_high, few_low, many_high, many_low, out,
                 *scratch):
    fields, folded = scratch[:FIELDS], scratch[FIELDS:]
    high0, low0, high1, low1 = folded
    for field in fields:
        field[...] = jnp.zeros(field.shape, F32)
    lane = lax.broadcasted_iota(jnp.int32, (1, 128), 1)

    def block(index, carry):
        count = counts[index]

        def some(begin, step):
            for k in range(begin, begin + step):
                cell = cells[index, k]
                value = weights[index, k]
                row = lax.shift_right_logical(cell, 7)
                here = lane == (jnp.full((1, 128), cell, jnp.int32) & 127)
                fields[k % FIELDS][pl.ds(row, 1), :] += jnp.where(here, value, 0.0)

        def halves(begin, size):
            @pl.when(count > begin)
            def _():
                if size == 16:
                    some(begin, size)
                else:
                    halves(begin, size // 2)
                    halves(begin + size // 2, size // 2)

        halves(0, SLOTS)
        return carry

    lax.fori_loop(0, counts.shape[0], block, 0)
    for a in range(3):
        for a2 in range(3):
            parts = []
            for part in range(3):
                tiles = []
                for b in range(16):
                    row = (16 * a + b) * CY + 8 * a2
                    tile = fields[0][pl.ds(row * 3 + part, 8, stride=3), :]
                    for field in fields[1:]:
                        tile = tile + field[pl.ds(row * 3 + part, 8, stride=3), :]
                    tiles.append(tile)
                parts.append(jnp.concatenate(tiles, axis=0))
            at = slice((a * 3 + a2) * 128, (a * 3 + a2 + 1) * 128)
            store_folded(folded, at, fold(parts))
    pitch = 2 * WIDTH
    half = N_DEV // 2
    first = lax.broadcasted_iota(jnp.int32, (half, NG), 0) == 0
    for a in range(3):
        at = slice(a * NG, (a + 1) * NG)
        value = dot3((many_high[...], many_low[...]), (high1[at, :], low1[at, :]), NT)
        for c in range(2):
            plane = value[c * N_DEV : (c + 1) * N_DEV]
            store_plane(out, WIDTH + c * LB + 3 * a, pitch, plane)
        dens_cos, dens_sin = z_density[:half, at], z_density[half:, at]
        value = dot3((few_high[...], few_low[...]), (high0[at, :], low0[at, :]), NT)
        phot_cos, phot_sin = value[:half], value[half:]
        low_rows, top_rows = 3 * a, half * pitch + 3 * a
        store_plane(out, low_rows, pitch, jnp.where(first, phot_cos, dens_cos))
        store_plane(out, low_rows + LB, pitch, jnp.where(first, dens_cos, dens_sin))
        store_plane(out, top_rows, pitch, jnp.where(first, phot_sin, phot_cos))
        store_plane(out, top_rows + LB, pitch, jnp.where(first, dens_sin, phot_sin))


def three(re, im, sign):
    t_re, t_im = re[1] + re[2], im[1] + im[2]
    d_re = (re[1] - re[2]) * (sign * HALF_ROOT3)
    d_im = (im[1] - im[2]) * (sign * HALF_ROOT3)
    m_re, m_im = re[0] - 0.5 * t_re, im[0] - 0.5 * t_im
    return (re[0] + t_re, m_re - d_im, m_re + d_im), (im[0] + t_im, m_im + d_re, m_im - d_re)


def nine(re, im, sign):
    for group in [(0, 1, 2), (3, 4, 5), (6, 7, 8), (0, 3, 6), (1, 4, 7), (2, 5, 8)]:
        new_re, new_im = three([re[g] for g in group], [im[g] for g in group], sign)
        for k, g in enumerate(group):
            re[g], im[g] = new_re[k], new_im[k]


def middle_kernel(planes, got, *rest):
    count = len(TABLE_SHAPES) + planes - 1
    sources, out, rest = rest[:count], rest[count], rest[count + 1 :]
    tables, (tw1, work, r_high, r_low, l_high, l_low, back, sems) = rest[:count], rest[count:]
    dev_high, dev_low, tw_x, tw_y, tw2 = tables[:5]
    lane_high, lane_low, win, lane_back_high, lane_back_low = tables[5:10]
    dev_back_high, dev_back_low = tables[10:12]
    copies = [
        pltpu.make_async_copy(source, table, sems.at[k])
        for k, (source, table) in enumerate(zip(sources, tables))
    ]
    for copy in copies:
        copy.start()
    first_plane, out_pitch = (1, PITCH) if planes == 2 else (0, WIDTH)
    pitch = planes * WIDTH
    for p in range(planes):
        for c in range(2):
            for j in range(LB):
                high, low = split(got[pl.ds((p * 2 + c) * LB + j, N_DEV, stride=pitch), :])
                at, to = slice(c * N_DEV, (c + 1) * N_DEV), slice(j * 128, (j + 1) * 128)
                r_high[p, at, to] = high
                r_low[p, at, to] = low

    def dev():
        return dev_high[...], dev_low[...]

    def dev_back():
        return dev_back_high[...], dev_back_low[...]

    def mat():
        return lane_high[...], lane_low[...]

    def mat_back():
        return lane_back_high[...], lane_back_low[...]

    def arrive(stage):
        if stage < 3:
            for copy in copies[(0, 2, 5)[stage] : (2, 5, len(copies))[stage]]:
                copy.wait()
        if stage == 3 and planes == 2:
            for j in range(WIDTH):
                rows = pl.ds(j, N_DEV, stride=WIDTH)
                out[pl.ds(j, N_DEV, stride=PITCH), :] = tables[12][rows, :]
        if stage == 1:
            for k in range(N_PX):
                cos_x, sin_x = tw_x[0, k : k + 1, :], tw_x[1, k : k + 1, :]
                cos_y, sin_y = tw_y[0], tw_y[1]
                at = slice(k * N_PY, (k + 1) * N_PY)
                tw1[0, at, :] = cos_x * cos_y - sin_x * sin_y
                tw1[1, at, :] = sin_x * cos_y + cos_x * sin_y

    def across(p, k):
        at = slice(k * 256, min((k + 1) * 256, ROWS))
        work[p, :, at] = dot3(dev(), (r_high[p, :, at], r_low[p, :, at]))

    def row_block(block, offset=0):
        if isinstance(block, int):
            return slice(block * 16 + offset, block * 16 + offset + 16)
        return pl.ds(pl.multiple_of(block * 16 + offset, 16), 16)

    def forward(p, block):
        rows, rows_im = row_block(block), row_block(block, N_DEV)
        re, im = [], []
        for j in range(LB):
            at = slice(j * 128, (j + 1) * 128)
            cos, sin = tw1[0, rows, at], tw1[1, rows, at]
            x, y = work[p, rows, at], work[p, rows_im, at]
            re.append(x * cos + y * sin)
            im.append(y * cos - x * sin)
        nine(re, im, -1.0)
        for j in range(LB):
            at = slice(j * 128, (j + 1) * 128)
            cos, sin = tw2[0:1, at], tw2[1:2, at]
            to = row_block(block, j * N_DEV)
            l_high[p, to, :128], l_low[p, to, :128] = split(re[j] * cos + im[j] * sin)
            l_high[p, to, 128:], l_low[p, to, 128:] = split(im[j] * cos - re[j] * sin)

    def along(p, k):
        at = slice(k * NG, (k + 1) * NG)
        value = dot3((l_high[p, at, :], l_low[p, at, :]), mat())
        w = win[planes - 1 - p, at, :]
        l_high[p, at, :128], l_low[p, at, :128] = split(value[:, :128] * w)
        l_high[p, at, 128:], l_low[p, at, 128:] = split(value[:, 128:] * w)
        back[p, at, :] = dot3((l_high[p, at, :], l_low[p, at, :]), mat_back())

    def backward(p, block):
        rows, rows_im = row_block(block), row_block(block, N_DEV)
        re, im = [], []
        for j in range(LB):
            at = slice(j * 128, (j + 1) * 128)
            cos, sin = tw2[0:1, at], tw2[1:2, at]
            of = row_block(block, j * N_DEV)
            x, y = back[p, of, :128], back[p, of, 128:]
            re.append(x * cos - y * sin)
            im.append(y * cos + x * sin)
        nine(re, im, 1.0)
        for j in range(LB):
            at = slice(j * 128, (j + 1) * 128)
            cos, sin = tw1[0, rows, at], tw1[1, rows, at]
            r_high[p, rows, at], r_low[p, rows, at] = split(re[j] * cos - im[j] * sin)
            r_high[p, rows_im, at], r_low[p, rows_im, at] = split(im[j] * cos + re[j] * sin)

    def home(p, k):
        at = slice(k * 256, min((k + 1) * 256, ROWS))
        value = dot3(dev_back(), (r_high[p, :, at], r_low[p, :, at]))
        for c in range(2):
            start = (first_plane + p) * WIDTH + c * LB + k * 2
            store_plane(out, start, out_pitch, value[c * N_DEV : (c + 1) * N_DEV])

    stages = [(across, 5), (forward, N_PX), (along, 3), (backward, N_PX), (home, 5)]
    if planes == 1:
        for stage, (work_of, parts) in enumerate(stages):
            arrive(stage)
            if parts == N_PX:

                def step(block, carry, work_of=work_of):
                    work_of(0, block)
                    return carry

                lax.fori_loop(0, parts, step, 0)
            else:
                for part in range(parts):
                    work_of(0, part)
        return
    for stage in range(len(stages) + 1):
        arrive(stage)
        both = []
        for p in range(2):
            if 0 <= stage - p < len(stages):
                work_of, parts = stages[stage - p]
                both += [((k + 0.5) / parts, p, work_of, k) for k in range(parts)]
        for _, p, work_of, part in sorted(both, key=lambda item: item[:2]):
            work_of(p, part)


def z_last_kernel(got, few_high, few_low, many_high, many_low, out):
    a = pl.program_id(0)
    half = N_DEV // 2
    first = lax.broadcasted_iota(jnp.int32, (half, 128), 0) == 0
    many, few = [[], []], [[], []]
    for a2 in range(3):

        def load(plane, c, begin=0, count=N_DEV):
            start = begin * PITCH + (plane * 2 + c) * LB + a * 3 + a2
            return got[pl.ds(start, count, stride=PITCH), :]

        re_low, im_low = load(1, 0, 0, half), load(1, 1, 0, half)
        re_top, im_top = load(1, 0, half, half), load(1, 1, half, half)
        many[0].append(jnp.concatenate([load(0, 0), load(0, 1)], axis=0))
        many[1].append(jnp.concatenate([load(2, 0), load(2, 1)], axis=0))
        dens = [jnp.where(first, im_low, re_low), jnp.where(first, im_top, im_low)]
        phot = [jnp.where(first, re_low, re_top), jnp.where(first, re_top, im_top)]
        few[0].append(jnp.concatenate(dens, axis=0))
        few[1].append(jnp.concatenate(phot, axis=0))
    smooth = []
    for k in range(2):
        same = dot3(split(jnp.concatenate(few[k], axis=1)), (few_high[...], few_low[...]), TN)
        turn = dot3(split(jnp.concatenate(many[k], axis=1)), (many_high[...], many_low[...]), TN)
        even, odd = turn[:, :128], turn[:, 128:] * HALF_ROOT3
        rest = same - 0.5 * even
        smooth.append((same + even, rest + odd, rest - odd))
    for k in range(3):
        value = jnp.clip(smooth[1][k] / jnp.maximum(smooth[0][k], 0.5), 0.0, 1.0)
        for a2 in range(3):
            block = value[a2 * 128 : (a2 + 1) * 128].reshape(16, 8, 128)
            out[:, a2 * 8 : (a2 + 1) * 8, k * 128 : (k + 1) * 128] = block


SQUARE = [((256, 256), BF)] * 2
TABLE_SHAPES = [
    *SQUARE,
    ((2, N_PX, ROWS), F32),
    ((2, N_PY, ROWS), F32),
    ((8, ROWS), F32),
    *SQUARE,
    ((2, ROWS, 128), F32),
    *SQUARE,
    *SQUARE,
]
FOLDED = [pltpu.VMEM((ROWS, width), BF) for width in (128, 128, 256, 256)]


def placed_in(space, *arrays):
    return [pltpu.with_memory_space_constraint(jnp.asarray(a), space) for a in arrays]


def limit(mib):
    return pltpu.CompilerParams(vmem_limit_bytes=mib * 2**20)


def exchange(rows):
    send = rows.reshape(N_DEV, 1, rows.size // N_DEV)
    return lax.all_to_all(send, AXES, 0, 0, tiled=True).reshape(rows.shape)


def middle(got, planes, sources):
    shapes = TABLE_SHAPES + [(source.shape, F32) for source in sources[len(TABLE_SHAPES) :]]
    if planes == 2:
        out_shape = pltpu.VMEM((N_DEV * PITCH, 128), F32)
    else:
        out_shape = jax.ShapeDtypeStruct((N_DEV * WIDTH, 128), F32)
    return pl.pallas_call(
        functools.partial(middle_kernel, planes),
        out_shape=out_shape,
        in_specs=[pl.BlockSpec(memory_space=pltpu.VMEM)]
        + [pl.BlockSpec(memory_space=pl.ANY)] * len(shapes),
        scratch_shapes=[pltpu.VMEM(*shape) for shape in shapes]
        + [
            pltpu.VMEM((2, N_DEV, ROWS), F32),
            pltpu.VMEM((planes, 2 * N_DEV, ROWS), F32),
            pltpu.VMEM((planes, 2 * N_DEV, ROWS), BF),
            pltpu.VMEM((planes, 2 * N_DEV, ROWS), BF),
            pltpu.VMEM((planes, ROWS, 256), BF),
            pltpu.VMEM((planes, ROWS, 256), BF),
            pltpu.VMEM((planes, ROWS, 256), F32),
            pltpu.SemaphoreType.DMA((len(shapes),)),
        ],
        compiler_params=limit(24),
        name=f"middle{planes}",
    )(*placed_in(pltpu.VMEM, got), *placed_in(pltpu.HBM, *sources))


def on_device(photons, halo_cells, halo_counts, owners, density):
    table = z_tables()
    dev, dev_back = device_table()
    lane, lane_back = lane_table()
    tw = twiddles()

    send = pl.pallas_call(
        sort_kernel,
        out_shape=jax.ShapeDtypeStruct((N_PY * CAP * 2, SLOTS), F32),
        name="sort",
    )(photons, halo_cells, halo_counts.reshape(1, -1), owners.reshape(1, -1))
    halos = lax.all_to_all(send.reshape(N_PY, 2 * CAP, SLOTS), "py", 0, 0, tiled=True)

    send_a, few = pl.pallas_call(
        z_density_kernel,
        out_shape=(
            jax.ShapeDtypeStruct((N_DEV * WIDTH, 128), F32),
            jax.ShapeDtypeStruct((N_DEV, ROWS), F32),
        ),
        scratch_shapes=FOLDED,
        name="zdensity",
    )(density, *table)
    send_a, halos = lax.optimization_barrier((send_a, halos))
    got_a = exchange(send_a)

    halos = halos.reshape(N_PY * CAP, 2, SLOTS)
    weights, cells = halos[:, 0], halos[:, 1].astype(jnp.int32)
    slot = jnp.arange(1, SLOTS + 1, dtype=jnp.int32)[None, :]
    counts = jnp.max(jnp.where(weights != 0, slot, 0), axis=1)
    smem = pl.BlockSpec(memory_space=pltpu.SMEM)
    vmem = pl.BlockSpec(memory_space=pltpu.VMEM)
    send_bc = pl.pallas_call(
        paint_kernel,
        out_shape=jax.ShapeDtypeStruct((N_DEV * 2 * WIDTH, 128), F32),
        in_specs=[smem, smem, smem] + [vmem] * 5,
        scratch_shapes=[pltpu.VMEM((ROWS * 3, 128), F32)] * FIELDS
        + FOLDED,
        name="paint",
    )(weights, cells, counts, few, *table)
    got_bc = exchange(send_bc)

    me = lax.axis_index(AXES)
    half = N_DEV // 2
    high = 3 * me // 2 + 1
    low = jnp.where(me % half == 0, (me // half) * (NG // 2), 3 * (me % half))
    win = pl.pallas_call(
        window_kernel,
        out_shape=jax.ShapeDtypeStruct((2, ROWS, 128), F32),
        in_specs=[smem],
        name="window",
    )(jnp.stack([high, low]).astype(jnp.int32))
    tables = (*dev, *tw, *lane, win, *lane_back, *dev_back)
    back_a = middle(got_a, 1, tables)
    back = middle(got_bc, 2, (*tables, back_a))
    got = exchange(back)
    whole = pl.BlockSpec((N_DEV * PITCH, 128), lambda i: (0, 0))
    whole_t = [pl.BlockSpec(t.shape, lambda i: (0, 0)) for t in table]
    return pl.pallas_call(
        z_last_kernel,
        grid=(3,),
        in_specs=[whole] + whole_t,
        out_specs=pl.BlockSpec((16, CY, NG), lambda i: (i, 0, 0)),
        out_shape=jax.ShapeDtypeStruct((CX, CY, NG), F32),
        compiler_params=limit(16),
        name="zlast",
    )(*placed_in(pltpu.VMEM, got, *table))


def solution(mesh):
    placed = (
        P(("px", "py"), None),
        P(("px", "py"), None),
        P(("px", "py")),
        P(("px", "py"), None),
        P("px", "py", None),
    )
    return jax.shard_map(
        on_device, mesh=mesh, in_specs=placed, out_specs=P("px", "py", None), check_vma=False
    )
```

```python
import functools
import math

import jax
import jax.numpy as jnp
import ml_dtypes
import numpy as np
from jax import lax
from jax.experimental import pallas as pl
from jax.experimental.pallas import tpu as pltpu
from jax.sharding import PartitionSpec as P

NG = 384
SLOTS = 128
CAP = 4
RADIUS = 20
N_PX = 8
N_PY = 16
N_DEV = 128
CX = 48
CY = 24
ROWS = CX * CY
LB = ROWS // 128
PLANES = 3
WIDTH = 2 * LB
PITCH = PLANES * WIDTH
FIELDS = 4
AXES = ("px", "py")
BF = jnp.bfloat16
F32 = jnp.float32
NT = ((1,), (1,))
NN = ((1,), (0,))
TN = ((0,), (0,))
HALF_ROOT3 = math.sqrt(3.0) / 2.0

LANE_A, LANE_A2, LANE_B, LANE_Y = (
    g.reshape(-1) for g in np.meshgrid(range(3), range(3), range(16), range(8), indexing="ij")
)
LANE_CX = 16 * LANE_A + LANE_B
LANE_CY = 8 * LANE_A2 + LANE_Y


def split_np(table):
    high = table.astype(ml_dtypes.bfloat16)
    low = (table - high.astype(np.float64)).astype(ml_dtypes.bfloat16)
    return high, low


def z_tables():
    z = np.arange(128)
    kz = 3 * np.arange(N_DEV // 2)
    angle = 2.0 * np.pi * (np.outer(kz, z) % NG) / NG
    few = np.concatenate([np.cos(angle), np.sin(angle)])
    few[N_DEV // 2] = 1.0 - 2.0 * (z % 2)
    kz = 3 * np.arange(N_DEV) // 2 + 1
    angle = 2.0 * np.pi * (np.outer(kz, z) % NG) / NG
    sign = np.where(kz % 3 == 1, 1.0, -1.0)[:, None]
    cos, sin = np.cos(angle), np.sin(angle)
    many = np.block([[cos, -sign * sin], [sin, sign * cos]])
    return (*split_np(few), *split_np(many))


def real_form(frac):
    angle = 2.0 * np.pi * (frac % 1.0)
    cos, sin = np.cos(angle), np.sin(angle)
    return np.block([[cos, sin], [-sin, cos]])


def device_table():
    s = np.arange(N_DEV)
    i, q = s // N_PY, s % N_PY
    form = real_form(np.outer(i, i) / N_PX + np.outer(q, q) / N_PY)
    return split_np(form), split_np(form.T)


def lane_table():
    m = np.arange(128)
    b, y = m // 8, m % 8
    form = real_form(np.outer(b, b) / 16.0 + np.outer(y, y) / 8.0)
    return split_np(form.T), split_np(form)


def twiddles():
    angle_x = 2.0 * np.pi * np.outer(np.arange(N_PX), LANE_CX) / NG
    angle_y = 2.0 * np.pi * np.outer(np.arange(N_PY), LANE_CY) / NG
    tw_x = np.stack([np.cos(angle_x), np.sin(angle_x)]).astype(np.float32)
    tw_y = np.stack([np.cos(angle_y), np.sin(angle_y)]).astype(np.float32)
    angle2 = 2.0 * np.pi * (LANE_B * LANE_A / 48.0 + LANE_Y * LANE_A2 / 24.0)
    tw2 = np.zeros((8, ROWS), np.float32)
    tw2[0], tw2[1] = np.cos(angle2), np.sin(angle2)
    return tw_x, tw_y, tw2


def split(value):
    high = value.astype(BF)
    return high, (value - high.astype(F32)).astype(BF)


def dot(left, right, dims=NN):
    return lax.dot_general(left, right, (dims, ((), ())), preferred_element_type=F32)


def dot3(left, right, dims=NN):
    (left_dim,), (right_dim,) = dims
    return dot(
        jnp.concatenate([left[0], left[1], left[0]], axis=left_dim),
        jnp.concatenate([right[0], right[0], right[1]], axis=right_dim),
        dims,
    )


def window_kernel(kz_ref, out):
    step = 64

    def block(index, carry):
        kz = kz_ref[index // (ROWS // step)]
        begin = pl.multiple_of((index % (ROWS // step)) * step, step)
        row = lax.broadcasted_iota(jnp.int32, (step, 128), 0) + begin
        lane = lax.broadcasted_iota(jnp.int32, (step, 128), 1)
        u, k1 = begin // N_DEV, row & (N_DEV - 1)
        kx = (k1 >> 4) + N_PX * (u // 3 + 3 * (lane >> 3))
        ky = (k1 & 15) + N_PY * (u % 3 + 3 * (lane & 7))
        fx = jnp.where(kx < NG // 2, kx, kx - NG)
        fy = jnp.where(ky < NG // 2, ky, ky - NG)
        square = (fx * fx + fy * fy + kz * kz).astype(F32)
        radial = jnp.sqrt(square) * (2.0 * math.pi * RADIUS / NG)
        safe = jnp.where(radial > 0, radial, 1.0)
        value = 3.0 * (jnp.sin(safe) - safe * jnp.cos(safe)) / (safe * safe * safe)
        value = jnp.where(radial > 0, value, 1.0)
        both = (kz > 0) & (kz < NG // 2)
        scale = jnp.where(both, 2.0 / float(NG) ** 3, 1.0 / float(NG) ** 3)
        out[index // (ROWS // step), pl.ds(begin, step), :] = value * scale
        return carry

    lax.fori_loop(0, 2 * ROWS // step, block, 0)


def sort_kernel(photons, cells, counts, owners, out):
    blocks = photons.shape[0]
    slots = N_PY * CAP
    target = owners[...]
    hot = jnp.where(
        lax.broadcasted_iota(jnp.int32, (N_PY, blocks), 0) == target, 1.0, 0.0
    )
    before = jnp.where(
        lax.broadcasted_iota(jnp.int32, (blocks, blocks), 0)
        < lax.broadcasted_iota(jnp.int32, (blocks, blocks), 1),
        1.0,
        0.0,
    )
    rank = jnp.sum(dot(hot.astype(BF), before.astype(BF)) * hot, axis=0, keepdims=True)
    place = target * CAP + rank.astype(jnp.int32)
    place_hot = jnp.where(
        lax.broadcasted_iota(jnp.int32, (slots, blocks), 0) == place, 1.0, 0.0
    )
    count = jnp.sum(place_hot * counts[...].astype(F32), axis=1, keepdims=True)
    live = lax.broadcasted_iota(jnp.int32, (slots, SLOTS), 1) < count.astype(jnp.int32)
    place_hot = place_hot.astype(BF)
    for half, value in enumerate((photons[...], cells[...].astype(F32))):
        rest, total = value, None
        for _ in range(3):
            first = rest.astype(BF)
            rest = rest - first.astype(F32)
            part = dot(place_hot, first)
            total = part if total is None else total + part
        out[pl.ds(half, slots, stride=2), :] = jnp.where(live, total, 0.0)


def fold(parts):
    t = parts[1] + parts[2]
    return parts[0] + t, parts[0] - 0.5 * t, (parts[1] - parts[2]) * HALF_ROOT3


def z_density_kernel(density, few_high, few_low, many_high, many_low, out, few, *scratch):
    high0, low0, high1, low1 = scratch
    for a in range(3):
        for a2 in range(3):
            at = slice((a * 3 + a2) * 128, (a * 3 + a2 + 1) * 128)
            block = density[a * 16 : (a + 1) * 16, a2 * 8 : (a2 + 1) * 8, :].reshape(128, NG)
            store_folded(scratch, at, fold([block[:, k * 128 : (k + 1) * 128] for k in range(3)]))
    for a in range(3):
        at = slice(a * NG, (a + 1) * NG)
        value = dot3((many_high[...], many_low[...]), (high1[at, :], low1[at, :]), NT)
        for c in range(2):
            store_plane(out, c * LB + 3 * a, WIDTH, value[c * N_DEV : (c + 1) * N_DEV])
        few[:, at] = dot3((few_high[...], few_low[...]), (high0[at, :], low0[at, :]), NT)


def store_folded(scratch, at, folded):
    high0, low0, high1, low1 = scratch
    high0[at, :], low0[at, :] = split(folded[0])
    high1[at, :128], low1[at, :128] = split(folded[1])
    high1[at, 128:], low1[at, 128:] = split(folded[2])


def store_plane(out, start, pitch, value):
    for j in range(value.shape[1] // 128):
        rows = pl.ds(start + j, value.shape[0], stride=pitch)
        out[rows, :] = value[:, j * 128 : (j + 1) * 128]


def paint_kernel(weights, cells, counts, z_density, few_high, few_low, many_high, many_low, out,
                 *scratch):
    fields, folded = scratch[:FIELDS], scratch[FIELDS:]
    high0, low0, high1, low1 = folded
    for field in fields:
        field[...] = jnp.zeros(field.shape, F32)
    lane = lax.broadcasted_iota(jnp.int32, (1, 128), 1)

    def block(index, carry):
        count = counts[index]

        def some(begin, step):
            for k in range(begin, begin + step):
                cell = cells[index, k]
                value = weights[index, k]
                row = lax.shift_right_logical(cell, 7)
                here = lane == (jnp.full((1, 128), cell, jnp.int32) & 127)
                fields[k % FIELDS][pl.ds(row, 1), :] += jnp.where(here, value, 0.0)

        def halves(begin, size):
            @pl.when(count > begin)
            def _():
                if size == 16:
                    some(begin, size)
                else:
                    halves(begin, size // 2)
                    halves(begin + size // 2, size // 2)

        halves(0, SLOTS)
        return carry

    lax.fori_loop(0, counts.shape[0], block, 0)
    for a in range(3):
        for a2 in range(3):
            parts = []
            for part in range(3):
                tiles = []
                for b in range(16):
                    row = (16 * a + b) * CY + 8 * a2
                    tile = fields[0][pl.ds(row * 3 + part, 8, stride=3), :]
                    for field in fields[1:]:
                        tile = tile + field[pl.ds(row * 3 + part, 8, stride=3), :]
                    tiles.append(tile)
                parts.append(jnp.concatenate(tiles, axis=0))
            at = slice((a * 3 + a2) * 128, (a * 3 + a2 + 1) * 128)
            store_folded(folded, at, fold(parts))
    pitch = 2 * WIDTH
    half = N_DEV // 2
    first = lax.broadcasted_iota(jnp.int32, (half, NG), 0) == 0
    for a in range(3):
        at = slice(a * NG, (a + 1) * NG)
        value = dot3((many_high[...], many_low[...]), (high1[at, :], low1[at, :]), NT)
        for c in range(2):
            plane = value[c * N_DEV : (c + 1) * N_DEV]
            store_plane(out, WIDTH + c * LB + 3 * a, pitch, plane)
        dens_cos, dens_sin = z_density[:half, at], z_density[half:, at]
        value = dot3((few_high[...], few_low[...]), (high0[at, :], low0[at, :]), NT)
        phot_cos, phot_sin = value[:half], value[half:]
        low_rows, top_rows = 3 * a, half * pitch + 3 * a
        store_plane(out, low_rows, pitch, jnp.where(first, phot_cos, dens_cos))
        store_plane(out, low_rows + LB, pitch, jnp.where(first, dens_cos, dens_sin))
        store_plane(out, top_rows, pitch, jnp.where(first, phot_sin, phot_cos))
        store_plane(out, top_rows + LB, pitch, jnp.where(first, dens_sin, phot_sin))


def three(re, im, sign):
    t_re, t_im = re[1] + re[2], im[1] + im[2]
    d_re = (re[1] - re[2]) * (sign * HALF_ROOT3)
    d_im = (im[1] - im[2]) * (sign * HALF_ROOT3)
    m_re, m_im = re[0] - 0.5 * t_re, im[0] - 0.5 * t_im
    return (re[0] + t_re, m_re - d_im, m_re + d_im), (im[0] + t_im, m_im + d_re, m_im - d_re)


def nine(re, im, sign):
    for group in [(0, 1, 2), (3, 4, 5), (6, 7, 8), (0, 3, 6), (1, 4, 7), (2, 5, 8)]:
        new_re, new_im = three([re[g] for g in group], [im[g] for g in group], sign)
        for k, g in enumerate(group):
            re[g], im[g] = new_re[k], new_im[k]


def middle_kernel(planes, got, *rest):
    count = len(TABLE_SHAPES) + planes - 1
    sources, out, rest = rest[:count], rest[count], rest[count + 1 :]
    tables, (tw1, work, r_high, r_low, l_high, l_low, back, sems) = rest[:count], rest[count:]
    dev_high, dev_low, tw_x, tw_y, tw2 = tables[:5]
    lane_high, lane_low, win, lane_back_high, lane_back_low = tables[5:10]
    dev_back_high, dev_back_low = tables[10:12]
    copies = [
        pltpu.make_async_copy(source, table, sems.at[k])
        for k, (source, table) in enumerate(zip(sources, tables))
    ]
    for copy in copies:
        copy.start()
    first_plane, out_pitch = (1, PITCH) if planes == 2 else (0, WIDTH)
    pitch = planes * WIDTH

    def assemble(p, j):
        for c in range(2):
            high, low = split(got[pl.ds((p * 2 + c) * LB + j, N_DEV, stride=pitch), :])
            at, to = slice(c * N_DEV, (c + 1) * N_DEV), slice(j * 128, (j + 1) * 128)
            r_high[p, at, to] = high
            r_low[p, at, to] = low

    def dev():
        return dev_high[...], dev_low[...]

    def dev_back():
        return dev_back_high[...], dev_back_low[...]

    def mat():
        return lane_high[...], lane_low[...]

    def mat_back():
        return lane_back_high[...], lane_back_low[...]

    def arrive(stage):
        if stage < 4:
            for copy in copies[(0, 0, 2, 5)[stage] : (0, 2, 5, len(copies))[stage]]:
                copy.wait()
        if stage == 4 and planes == 2:
            for j in range(WIDTH):
                rows = pl.ds(j, N_DEV, stride=WIDTH)
                out[pl.ds(j, N_DEV, stride=PITCH), :] = tables[12][rows, :]
        if stage == 2:
            for k in range(N_PX):
                cos_x, sin_x = tw_x[0, k : k + 1, :], tw_x[1, k : k + 1, :]
                cos_y, sin_y = tw_y[0], tw_y[1]
                at = slice(k * N_PY, (k + 1) * N_PY)
                tw1[0, at, :] = cos_x * cos_y - sin_x * sin_y
                tw1[1, at, :] = sin_x * cos_y + cos_x * sin_y

    def across(p, k):
        at = slice(k * 256, min((k + 1) * 256, ROWS))
        work[p, :, at] = dot3(dev(), (r_high[p, :, at], r_low[p, :, at]))

    def row_block(block, offset=0):
        if isinstance(block, int):
            return slice(block * 16 + offset, block * 16 + offset + 16)
        return pl.ds(pl.multiple_of(block * 16 + offset, 16), 16)

    def forward(p, block):
        rows, rows_im = row_block(block), row_block(block, N_DEV)
        re, im = [], []
        for j in range(LB):
            at = slice(j * 128, (j + 1) * 128)
            cos, sin = tw1[0, rows, at], tw1[1, rows, at]
            x, y = work[p, rows, at], work[p, rows_im, at]
            re.append(x * cos + y * sin)
            im.append(y * cos - x * sin)
        nine(re, im, -1.0)
        for j in range(LB):
            at = slice(j * 128, (j + 1) * 128)
            cos, sin = tw2[0:1, at], tw2[1:2, at]
            to = row_block(block, j * N_DEV)
            if j:
                re[j], im[j] = re[j] * cos + im[j] * sin, im[j] * cos - re[j] * sin
            l_high[p, to, :128], l_low[p, to, :128] = split(re[j])
            l_high[p, to, 128:], l_low[p, to, 128:] = split(im[j])

    def along(p, k):
        at = slice(k * NG, (k + 1) * NG)
        value = dot3((l_high[p, at, :], l_low[p, at, :]), mat())
        w = win[planes - 1 - p, at, :]
        l_high[p, at, :128], l_low[p, at, :128] = split(value[:, :128] * w)
        l_high[p, at, 128:], l_low[p, at, 128:] = split(value[:, 128:] * w)
        back[p, at, :] = dot3((l_high[p, at, :], l_low[p, at, :]), mat_back())

    def backward(p, block):
        rows, rows_im = row_block(block), row_block(block, N_DEV)
        re, im = [], []
        for j in range(LB):
            at = slice(j * 128, (j + 1) * 128)
            cos, sin = tw2[0:1, at], tw2[1:2, at]
            of = row_block(block, j * N_DEV)
            x, y = back[p, of, :128], back[p, of, 128:]
            re.append(x * cos - y * sin if j else x)
            im.append(y * cos + x * sin if j else y)
        nine(re, im, 1.0)
        for j in range(LB):
            at = slice(j * 128, (j + 1) * 128)
            cos, sin = tw1[0, rows, at], tw1[1, rows, at]
            r_high[p, rows, at], r_low[p, rows, at] = split(re[j] * cos - im[j] * sin)
            r_high[p, rows_im, at], r_low[p, rows_im, at] = split(im[j] * cos + re[j] * sin)

    def home(p, k):
        at = slice(k * 256, min((k + 1) * 256, ROWS))
        value = dot3(dev_back(), (r_high[p, :, at], r_low[p, :, at]))
        for c in range(2):
            start = (first_plane + p) * WIDTH + c * LB + k * 2
            store_plane(out, start, out_pitch, value[c * N_DEV : (c + 1) * N_DEV])

    stages = [(assemble, LB), (across, 5), (forward, N_PX), (along, 3), (backward, N_PX), (home, 5)]
    if planes == 1:
        for stage, (work_of, parts) in enumerate(stages):
            arrive(stage)
            if parts == N_PX:

                def step(block, carry, work_of=work_of):
                    work_of(0, block)
                    return carry

                lax.fori_loop(0, parts, step, 0)
            else:
                for part in range(parts):
                    work_of(0, part)
        return
    for stage in range(len(stages) + 1):
        arrive(stage)
        both = []
        for p in range(2):
            if 0 <= stage - p < len(stages):
                work_of, parts = stages[stage - p]
                both += [((k + 0.5) / parts, p, work_of, k) for k in range(parts)]
        for _, p, work_of, part in sorted(both, key=lambda item: item[:2]):
            work_of(p, part)


def z_last_kernel(got, few_high, few_low, many_high, many_low, out):
    a = pl.program_id(0)
    half = N_DEV // 2
    first = lax.broadcasted_iota(jnp.int32, (half, 128), 0) == 0
    many, few = [[], []], [[], []]
    for a2 in range(3):

        def load(plane, c, begin=0, count=N_DEV):
            start = begin * PITCH + (plane * 2 + c) * LB + a * 3 + a2
            return got[pl.ds(start, count, stride=PITCH), :]

        re_low, im_low = load(1, 0, 0, half), load(1, 1, 0, half)
        re_top, im_top = load(1, 0, half, half), load(1, 1, half, half)
        many[0].append(jnp.concatenate([load(0, 0), load(0, 1)], axis=0))
        many[1].append(jnp.concatenate([load(2, 0), load(2, 1)], axis=0))
        dens = [jnp.where(first, im_low, re_low), jnp.where(first, im_top, im_low)]
        phot = [jnp.where(first, re_low, re_top), jnp.where(first, re_top, im_top)]
        few[0].append(jnp.concatenate(dens, axis=0))
        few[1].append(jnp.concatenate(phot, axis=0))
    smooth = []
    for k in range(2):
        same = dot3(split(jnp.concatenate(few[k], axis=1)), (few_high[...], few_low[...]), TN)
        turn = dot3(split(jnp.concatenate(many[k], axis=1)), (many_high[...], many_low[...]), TN)
        even, odd = turn[:, :128], turn[:, 128:] * HALF_ROOT3
        rest = same - 0.5 * even
        smooth.append((same + even, rest + odd, rest - odd))
    for k in range(3):
        value = jnp.clip(smooth[1][k] / jnp.maximum(smooth[0][k], 0.5), 0.0, 1.0)
        for a2 in range(3):
            block = value[a2 * 128 : (a2 + 1) * 128].reshape(16, 8, 128)
            out[:, a2 * 8 : (a2 + 1) * 8, k * 128 : (k + 1) * 128] = block


SQUARE = [((256, 256), BF)] * 2
TABLE_SHAPES = [
    *SQUARE,
    ((2, N_PX, ROWS), F32),
    ((2, N_PY, ROWS), F32),
    ((8, ROWS), F32),
    *SQUARE,
    ((2, ROWS, 128), F32),
    *SQUARE,
    *SQUARE,
]
FOLDED = [pltpu.VMEM((ROWS, width), BF) for width in (128, 128, 256, 256)]


def placed_in(space, *arrays):
    return [pltpu.with_memory_space_constraint(jnp.asarray(a), space) for a in arrays]


def limit(mib):
    return pltpu.CompilerParams(vmem_limit_bytes=mib * 2**20)


def exchange(rows):
    send = rows.reshape(N_DEV, 1, rows.size // N_DEV)
    return lax.all_to_all(send, AXES, 0, 0, tiled=True).reshape(rows.shape)


def middle(got, planes, sources):
    shapes = TABLE_SHAPES + [(source.shape, F32) for source in sources[len(TABLE_SHAPES) :]]
    if planes == 2:
        out_shape = pltpu.VMEM((N_DEV * PITCH, 128), F32)
    else:
        out_shape = jax.ShapeDtypeStruct((N_DEV * WIDTH, 128), F32)
    return pl.pallas_call(
        functools.partial(middle_kernel, planes),
        out_shape=out_shape,
        in_specs=[pl.BlockSpec(memory_space=pltpu.VMEM)]
        + [pl.BlockSpec(memory_space=pl.ANY)] * len(shapes),
        scratch_shapes=[pltpu.VMEM(*shape) for shape in shapes]
        + [
            pltpu.VMEM((2, N_DEV, ROWS), F32),
            pltpu.VMEM((planes, 2 * N_DEV, ROWS), F32),
            pltpu.VMEM((planes, 2 * N_DEV, ROWS), BF),
            pltpu.VMEM((planes, 2 * N_DEV, ROWS), BF),
            pltpu.VMEM((planes, ROWS, 256), BF),
            pltpu.VMEM((planes, ROWS, 256), BF),
            pltpu.VMEM((planes, ROWS, 256), F32),
            pltpu.SemaphoreType.DMA((len(shapes),)),
        ],
        compiler_params=limit(24),
        name=f"middle{planes}",
    )(*placed_in(pltpu.VMEM, got), *placed_in(pltpu.HBM, *sources))


def on_device(photons, halo_cells, halo_counts, owners, density):
    table = z_tables()
    dev, dev_back = device_table()
    lane, lane_back = lane_table()
    tw = twiddles()

    send = pl.pallas_call(
        sort_kernel,
        out_shape=jax.ShapeDtypeStruct((N_PY * CAP * 2, SLOTS), F32),
        name="sort",
    )(photons, halo_cells, halo_counts.reshape(1, -1), owners.reshape(1, -1))
    halos = lax.all_to_all(send.reshape(N_PY, 2 * CAP, SLOTS), "py", 0, 0, tiled=True)

    send_a, few = pl.pallas_call(
        z_density_kernel,
        out_shape=(
            jax.ShapeDtypeStruct((N_DEV * WIDTH, 128), F32),
            jax.ShapeDtypeStruct((N_DEV, ROWS), F32),
        ),
        scratch_shapes=FOLDED,
        name="zdensity",
    )(density, *table)
    send_a, halos = lax.optimization_barrier((send_a, halos))
    got_a = exchange(send_a)

    halos = halos.reshape(N_PY * CAP, 2, SLOTS)
    weights, cells = halos[:, 0], halos[:, 1].astype(jnp.int32)
    slot = jnp.arange(1, SLOTS + 1, dtype=jnp.int32)[None, :]
    counts = jnp.max(jnp.where(weights != 0, slot, 0), axis=1)
    smem = pl.BlockSpec(memory_space=pltpu.SMEM)
    vmem = pl.BlockSpec(memory_space=pltpu.VMEM)
    send_bc = pl.pallas_call(
        paint_kernel,
        out_shape=jax.ShapeDtypeStruct((N_DEV * 2 * WIDTH, 128), F32),
        in_specs=[smem, smem, smem] + [vmem] * 5,
        scratch_shapes=[pltpu.VMEM((ROWS * 3, 128), F32)] * FIELDS
        + FOLDED,
        name="paint",
    )(weights, cells, counts, few, *table)
    got_bc = exchange(send_bc)

    me = lax.axis_index(AXES)
    half = N_DEV // 2
    high = 3 * me // 2 + 1
    low = jnp.where(me % half == 0, (me // half) * (NG // 2), 3 * (me % half))
    win = pl.pallas_call(
        window_kernel,
        out_shape=jax.ShapeDtypeStruct((2, ROWS, 128), F32),
        in_specs=[smem],
        name="window",
    )(jnp.stack([high, low]).astype(jnp.int32))
    tables = (*dev, *tw, *lane, win, *lane_back, *dev_back)
    back_a = middle(got_a, 1, tables)
    back = middle(got_bc, 2, (*tables, back_a))
    got = exchange(back)
    whole = pl.BlockSpec((N_DEV * PITCH, 128), lambda i: (0, 0))
    whole_t = [pl.BlockSpec(t.shape, lambda i: (0, 0)) for t in table]
    return pl.pallas_call(
        z_last_kernel,
        grid=(3,),
        in_specs=[whole] + whole_t,
        out_specs=pl.BlockSpec((16, CY, NG), lambda i: (i, 0, 0)),
        out_shape=jax.ShapeDtypeStruct((CX, CY, NG), F32),
        compiler_params=limit(16),
        name="zlast",
    )(*placed_in(pltpu.VMEM, got, *table))


def solution(mesh):
    placed = (
        P(("px", "py"), None),
        P(("px", "py"), None),
        P(("px", "py")),
        P(("px", "py"), None),
        P("px", "py", None),
    )
    return jax.shard_map(
        on_device, mesh=mesh, in_specs=placed, out_specs=P("px", "py", None), check_vma=False
    )
```
